32 devices in a mesh: dp: 16 (over z, x, core), head: 2 (over y).
Axes of the slice: x: 2, y: 2, z: 4, core: 2. Of those that a mesh axis runs over, the one named last changes fastest.
Arguments:
- layer_in: bfloat16 [4096, 1536], P('dp'), may hold values from -6 to 6
- gain_attn: bfloat16 [1536], replicated, may hold values from 0.5 to 1.5
- q_weight: bfloat16 [1536, 1536], P('dp', 'head'), may hold values from -0.15625 to 0.15625
- q_bias: bfloat16 [1536], P('head'), may hold values from -3 to 3
- key_weight: bfloat16 [1536, 256], P('dp', 'head'), may hold values from -0.15625 to 0.15625
- key_bias: bfloat16 [256], P('head'), may hold values from -3 to 3
- value_weight: bfloat16 [1536, 256], P('dp', 'head'), may hold values from -0.15625 to 0.15625
- value_bias: bfloat16 [256], P('head'), may hold values from -3 to 3
- o_weight: bfloat16 [1536, 1536], P('head', 'dp'), may hold values from -0.875 to 0.875
- gain_mlp: bfloat16 [1536], replicated, may hold values from 0.5 to 1.5
- gate_weight: bfloat16 [1536, 8960], P('dp', 'head'), may hold values from -0.15625 to 0.15625
- up_weight: bfloat16 [1536, 8960], P('dp', 'head'), may hold values from -0.15625 to 0.15625
- down_weight: bfloat16 [8960, 1536], P('head', 'dp'), may hold values from -0.0625 to 0.0625
- row_lengths: int32 [3], replicated, may hold values from 1 to 2048, 4096 in all
- source_ids: int32 [4096], P('dp'), may hold values from 0 to 7
- source_weights: int32 [8], replicated, may hold values from 4 to 32
- out_grad: bfloat16 [4096, 1536], P('dp'), may hold values from -6 to 6
Outputs:
- layer_out: bfloat16 [4096, 1536], P('dp')
- layer_in_grad: bfloat16 [4096, 1536], P('dp')
- gain_attn_grad: float32 [1536], replicated
- q_weight_grad: float32 [1536, 1536], P('dp', 'head')
- q_bias_grad: float32 [1536], P('head')
- k_weight_grad: float32 [1536, 256], P('dp', 'head')
- k_bias_grad: float32 [256], P('head')
- v_weight_grad: float32 [1536, 256], P('dp', 'head')
- v_bias_grad: float32 [256], P('head')
- o_weight_grad: float32 [1536, 1536], P('head', 'dp')
- gain_mlp_grad: float32 [1536], replicated
- gate_weight_grad: float32 [1536, 8960], P('dp', 'head')
- up_weight_grad: float32 [1536, 8960], P('dp', 'head')
- down_weight_grad: float32 [8960, 1536], P('head', 'dp')
The draws below stay inside these ranges and needn't reach their ends.
Inputs may be any that keep to these rules, and one draw needn't show every extreme that they name: `row_lengths`: 3 document lengths that sum to 4096; the longest is exactly 2048. `source_weights`: numerators over the denominator 16.
All inputs are finite; a program needn't handle non-finite values.
Results may differ from the reference program's by a relative error of at most 0.025.
Values may be sent and summed in bfloat16 or wider, within the bound.
A program may use at most 256 MiB of HBM per device.

```python
import math
import jax
import jax.numpy as jnp
import numpy as np
from jax import lax

MODEL_WIDTH = 1536
QUERY_HEADS = 12
KEY_VALUE_HEADS = 2
HEAD_SIZE = 128
FF = 8960
BLOCK_TOKENS = 512
NSRC = 8
TOKENS = 4096
SEQ_MOST = 2048
NSEQ = 3


def plant(entries, rng, low, high):
    longest = entries.shape.index(max(entries.shape))
    spots = []
    for shift in (0, 1):
        where = [jax.random.randint(jax.random.fold_in(rng, axis), (), 0, length) for axis, length in enumerate(entries.shape)]
        where[longest] = (where[longest] + shift) % entries.shape[longest]
        spots.append(tuple(where))
    return entries.at[spots[0]].set(low).at[spots[1]].set(high)


def with_spikes(result, stream_key, source, target, parts, factor):
    owner, partner = [(jnp.arange(result.shape[position]) // (result.shape[position] // parts)).reshape([-1 if axis == position else 1 for axis in range(result.ndim)]) for position in (source, target)]
    chosen = jax.random.permutation(stream_key, parts)[partner]
    strong = (owner == chosen) | (owner == (partner + parts // 2) % parts)
    return jnp.where(strong, factor * result, result)


def block_levels(stream_key, shape, pieces, low, high):
    loudness = 1.0
    for position, parts in pieces:
        heights = jax.random.uniform(jax.random.fold_in(jax.random.fold_in(stream_key, 6), position), (parts,), jnp.float32, low / len(pieces), high / len(pieces))
        loudness = loudness * jnp.repeat(jnp.exp(heights), shape[position] // parts).reshape((-1,) + (1,) * (len(shape) - 1 - position))
    return loudness


def rank_table(number_of, slope):
    portions = [(1 << 20) // math.isqrt(standing ** slope) + 1 for standing in range(1, number_of + 1)]
    width = 1 + sum(portions) // (1 << 30)
    return np.cumsum(np.array([max(1, weight // width) for weight in portions]))


def skewed_ids(rng, extent, count, lean):
    table = rank_table(count, lean)
    pick = jax.random.randint(jax.random.fold_in(rng, 1), extent, 0, int(table[count - 1]))
    grade = jnp.searchsorted(jnp.asarray(table, jnp.int32), pick, side="right")
    return jax.random.permutation(jax.random.fold_in(rng, 2), count)[grade].astype(jnp.int32)


def split_up(number_of, total, most, slope):
    portions = [(1 << 20) // math.isqrt(grade ** slope) + 1 for grade in range(2, number_of + 1)]
    spare, counts = total - most - (number_of - 1), [1] * (number_of - 1)
    while spare > 0:
        candidates = [i for i in range(number_of - 1) if counts[i] < most]
        whole, remaining = sum([portions[i] for i in candidates]), spare
        for i in candidates:
            extra = min(most - counts[i], max(1, remaining * portions[i] // whole), spare)
            counts[i] = counts[i] + extra
            spare = spare - extra
    return np.array([most] + counts)


def uneven(rng, count, total, reach, lean):
    if count == 2:
        one = jax.random.randint(rng, (), max(1, total - reach), min(reach, total - 1) + 1)
        return jnp.stack([one, total - one])
    tallies = jnp.asarray(split_up(count, total, reach, lean), jnp.int32)
    pairs = (count - 1) // 2
    source_of, receiver = tallies[1:1 + 2 * pairs:2], tallies[2:2 + 2 * pairs:2]
    margin = jnp.minimum(source_of - 1, reach - receiver)
    passed = jax.random.randint(jax.random.fold_in(rng, 1), (pairs,), 0, 1 << 20) % (margin + 1)
    tallies = tallies.at[1:1 + 2 * pairs:2].set(source_of - passed).at[2:2 + 2 * pairs:2].set(receiver + passed)
    return tallies[jax.random.permutation(jax.random.fold_in(rng, 2), count)]


def normal_values(key, extent, width, most, pieces=(), kind=jnp.bfloat16):
    drawn = jax.random.normal(key, extent, jnp.float32) * width
    if len(pieces) > 0:
        drawn = block_levels(key, extent, pieces, -0.22, 0.18) * drawn
    return jnp.clip(drawn, min=-most, max=most).astype(kind)


def gaussian_with(stream_key, shape, width, limit, shards, heavy, kind=jnp.bfloat16):
    entries = width * jax.random.normal(stream_key, shape, jnp.float32)
    if shards:
        entries = entries * block_levels(stream_key, shape, shards, -0.22, 0.18)
    return jnp.clip(with_spikes(entries, jax.random.fold_in(stream_key, 3), *heavy), -limit, limit).astype(kind)


def setup_inputs(seed: int = 0) -> dict:
    splits = jax.random.split(jax.random.key(seed), 18)
    layer_in = gaussian_with(splits[0], (TOKENS, MODEL_WIDTH), 1.0, 6.0, ((0, 16),), (0, 1, 16, 2.0))
    gain_attn = jnp.clip(1.0 + 0.1 * jax.random.normal(splits[1], (MODEL_WIDTH,), jnp.float32), 0.5, 1.5).astype(jnp.bfloat16)
    q_weight = normal_values(splits[2], (MODEL_WIDTH, QUERY_HEADS * HEAD_SIZE), MODEL_WIDTH ** -0.5, 0.15625, ((0, 16), (1, 2)))
    q_bias = normal_values(splits[3], (QUERY_HEADS * HEAD_SIZE,), 0.5, 3.0, ((0, 2),))
    key_weight = normal_values(splits[4], (MODEL_WIDTH, KEY_VALUE_HEADS * HEAD_SIZE), MODEL_WIDTH ** -0.5, 0.15625, ((0, 16), (1, 2)))
    key_bias = normal_values(splits[5], (KEY_VALUE_HEADS * HEAD_SIZE,), 0.5, 3.0, ((0, 2),))
    value_weight = normal_values(splits[6], (MODEL_WIDTH, KEY_VALUE_HEADS * HEAD_SIZE), MODEL_WIDTH ** -0.5, 0.15625, ((0, 16), (1, 2)))
    value_bias = normal_values(splits[7], (KEY_VALUE_HEADS * HEAD_SIZE,), 0.5, 3.0, ((0, 2),))
    o_weight = normal_values(splits[8], (QUERY_HEADS * HEAD_SIZE, MODEL_WIDTH), (MODEL_WIDTH // 32) ** -0.5, 0.875, ((0, 2), (1, 16)))
    gain_mlp = jnp.clip(1.0 + 0.1 * jax.random.normal(splits[9], (MODEL_WIDTH,), jnp.float32), 0.5, 1.5).astype(jnp.bfloat16)
    gate_weight = normal_values(splits[10], (MODEL_WIDTH, FF), MODEL_WIDTH ** -0.5, 0.15625, ((0, 16), (1, 2)))
    up_weight = normal_values(splits[11], (MODEL_WIDTH, FF), MODEL_WIDTH ** -0.5, 0.15625, ((0, 16), (1, 2)))
    down_weight = normal_values(splits[12], (FF, MODEL_WIDTH), FF ** -0.5, 0.0625, ((0, 2), (1, 16)))
    row_lengths = uneven(splits[13], NSEQ, TOKENS, SEQ_MOST, 2).astype(jnp.int32)
    source_ids = plant(skewed_ids(splits[14], (TOKENS,), NSRC, 2), jax.random.fold_in(splits[14], 3), 0, NSRC - 1).astype(jnp.int32)
    source_weights = plant(jax.random.randint(splits[15], (NSRC,), 4, 33), jax.random.fold_in(splits[15], 1), 4, 32).astype(jnp.int32)
    out_grad = gaussian_with(splits[16], (TOKENS, MODEL_WIDTH), 1.0, 6.0, ((0, 16),), (0, 1, 16, 2.0))
    return dict(layer_in=layer_in, gain_attn=gain_attn, q_weight=q_weight, q_bias=q_bias, key_weight=key_weight, key_bias=key_bias, value_weight=value_weight, value_bias=value_bias, o_weight=o_weight, gain_mlp=gain_mlp, gate_weight=gate_weight, up_weight=up_weight, down_weight=down_weight, row_lengths=row_lengths, source_ids=source_ids, source_weights=source_weights, out_grad=out_grad)


@jax.custom_vjp
def lower_bound(v):
    return lax.optimization_barrier(v.astype(jnp.bfloat16)).astype(jnp.float32)

@jax.custom_vjp
def lower_bound_backward(v):
    return v

def low_keep(v):
    return (lower_bound(v), None)

def low_pass(kept, grad):
    return (grad,)

def back_keep(v):
    return (v, None)

def back_low(kept, grad):
    return (lower_bound(grad),)
lower_bound.defvjp(low_keep, low_pass)
lower_bound_backward.defvjp(back_keep, back_low)
norm_epsilon = 1e-06
rope_base = 1000000.0
loss_denominator = 16.0
masked_score = -1e+30
highest = lax.Precision.HIGHEST

def doc_layout(row_lengths, token_count):
    doc_ends = jnp.cumsum(row_lengths).astype(jnp.int32)
    doc_starts = (doc_ends - row_lengths).astype(jnp.int32)
    token_index = jnp.arange(token_count, dtype=jnp.int32)
    doc_id = lax.optimization_barrier(jnp.sum((doc_ends[None, :] <= token_index[:, None]).astype(jnp.int32), axis=1)).astype(jnp.int32)
    doc_begin = lax.optimization_barrier(jnp.max(jnp.where(doc_starts[None, :] <= token_index[:, None], doc_starts[None, :], 0), axis=1)).astype(jnp.int32)
    return (doc_id, token_index - doc_begin)

def rope_tables(positions):
    freq = rope_base ** (-jnp.arange(0, HEAD_SIZE, 2, dtype=jnp.float32) / HEAD_SIZE)
    angle = positions.astype(jnp.float32)[:, None] * freq[None, :]
    angle = jnp.concatenate([angle, angle], axis=1)
    return (jnp.cos(angle)[:, None, :], jnp.sin(angle)[:, None, :])

def rotary_apply(values, cosine_table, sine_table):
    half_width = values.shape[-1] // 2
    turned = jnp.concatenate([-values[..., half_width:], values[..., :half_width]], axis=-1)
    return values * cosine_table + turned * sine_table

def rms_scale(values):
    return lax.rsqrt(lax.optimization_barrier(jnp.mean(values * values, axis=-1, keepdims=True)) + norm_epsilon)

def attention(query_rows, key_matrix, value_matrix, doc_id):
    token_count = query_rows.shape[0]
    group_width = QUERY_HEADS // KEY_VALUE_HEADS
    padded_rows = SEQ_MOST
    window = SEQ_MOST + BLOCK_TOKENS
    score_scale = HEAD_SIZE ** (-0.5)
    keys_padded = jnp.concatenate([jnp.zeros((padded_rows, KEY_VALUE_HEADS, HEAD_SIZE), jnp.float32), key_matrix], axis=0)
    values_padded = jnp.concatenate([jnp.zeros((padded_rows, KEY_VALUE_HEADS, HEAD_SIZE), jnp.float32), value_matrix], axis=0)
    doc_pad = jnp.concatenate([jnp.full((padded_rows,), -1, jnp.int32), doc_id.astype(jnp.int32)], axis=0)
    block_total = token_count // BLOCK_TOKENS
    query_block_list = query_rows.reshape(block_total, BLOCK_TOKENS, KEY_VALUE_HEADS, group_width, HEAD_SIZE)
    doc_blocks = doc_id.reshape(block_total, BLOCK_TOKENS)
    block_starts = jnp.arange(block_total, dtype=jnp.int32) * BLOCK_TOKENS

    def one_block(inputs):
        block_query, block_doc, block_start = inputs
        near_keys = lax.dynamic_slice_in_dim(keys_padded, block_start, window, 0)
        near_values = lax.dynamic_slice_in_dim(values_padded, block_start, window, 0)
        near_doc = lax.dynamic_slice_in_dim(doc_pad, block_start, window, 0)
        key_index = block_start - padded_rows + jnp.arange(window, dtype=jnp.int32)
        query_index = block_start + jnp.arange(BLOCK_TOKENS, dtype=jnp.int32)
        visible = (near_doc[None, :] == block_doc[:, None]) & (key_index[None, :] <= query_index[:, None])
        scores = jnp.einsum('qgjd,kgd->gjqk', block_query, near_keys, precision=highest)
        scores = lower_bound_backward(scores * score_scale)
        scores = jnp.where(visible[None, None], scores, masked_score)
        row_max = lax.optimization_barrier(jnp.max(scores, axis=-1, keepdims=True))
        expo = jnp.exp(scores - row_max)
        weights = expo / lax.optimization_barrier(jnp.sum(expo, axis=-1, keepdims=True))
        mixed = jnp.einsum('gjqk,kgd->qgjd', lower_bound(weights), near_values, precision=highest)
        return mixed.reshape(BLOCK_TOKENS, QUERY_HEADS * HEAD_SIZE)
    mixed_all = lax.map(jax.checkpoint(one_block), (query_block_list, doc_blocks, block_starts))
    return mixed_all.reshape(token_count, QUERY_HEADS * HEAD_SIZE)

def layer_forward(layer_in, gain_attn, q_weight, q_bias, key_weight, key_bias, value_weight, value_bias, o_weight, gain_mlp, gate_weight, up_weight, down_weight, doc_id, cosine_table, sine_table):
    token_count = layer_in.shape[0]
    normed = lower_bound(layer_in * rms_scale(layer_in) * gain_attn)
    query_pre = lower_bound_backward(jnp.dot(normed, q_weight, precision=highest) + q_bias)
    key_unrotated = lower_bound_backward(jnp.dot(normed, key_weight, precision=highest) + key_bias)
    value_matrix = lower_bound(lower_bound_backward(jnp.dot(normed, value_weight, precision=highest) + value_bias))
    query_rows = lower_bound(lower_bound_backward(rotary_apply(query_pre.reshape(token_count, QUERY_HEADS, HEAD_SIZE), cosine_table, sine_table)))
    key_matrix = lower_bound(lower_bound_backward(rotary_apply(key_unrotated.reshape(token_count, KEY_VALUE_HEADS, HEAD_SIZE), cosine_table, sine_table)))
    value_matrix = value_matrix.reshape(token_count, KEY_VALUE_HEADS, HEAD_SIZE)
    attended = lower_bound(lower_bound_backward(attention(query_rows, key_matrix, value_matrix, doc_id)))
    branch = lower_bound_backward(jnp.dot(attended, o_weight, precision=highest))
    hidden = layer_in + branch
    normed_mlp = lower_bound(hidden * rms_scale(hidden) * gain_mlp)
    gate_act = lower_bound_backward(jnp.dot(normed_mlp, gate_weight, precision=highest))
    up_act = lower_bound_backward(jnp.dot(normed_mlp, up_weight, precision=highest))
    active = lower_bound(gate_act * jax.nn.sigmoid(gate_act) * up_act)
    return hidden + lower_bound_backward(jnp.dot(active, down_weight, precision=highest))

def reference(layer_in, gain_attn, q_weight, q_bias, key_weight, key_bias, value_weight, value_bias, o_weight, gain_mlp, gate_weight, up_weight, down_weight, row_lengths, source_ids, source_weights, out_grad):
    doc_id, positions = doc_layout(row_lengths, TOKENS)
    cosine_table, sine_table = rope_tables(positions)
    primals = tuple((item.astype(jnp.float32) for item in (layer_in, gain_attn, q_weight, q_bias, key_weight, key_bias, value_weight, value_bias, o_weight, gain_mlp, gate_weight, up_weight, down_weight)))

    def forward(*params):
        return layer_forward(*params, doc_id, cosine_table, sine_table)
    output, pullback = jax.vjp(forward, *primals)
    picked = source_ids[:, None] == jnp.arange(NSRC, dtype=jnp.int32)[None, :]
    row_scale = lax.optimization_barrier(jnp.sum(jnp.where(picked, source_weights[None, :], 0), axis=1)).astype(jnp.float32) / loss_denominator
    cotangent = out_grad.astype(jnp.float32) * row_scale[:, None]
    grads = pullback(cotangent)
    return (output.astype(jnp.bfloat16), grads[0].astype(jnp.bfloat16), grads[1], grads[2], grads[3], grads[4], grads[5], grads[6], grads[7], grads[8], grads[9], grads[10], grads[11], grads[12])
```

```python
import dataclasses
import functools
from typing import Any, Callable
import jax
import jax.numpy as jnp
from jax import lax
from jax.experimental import pallas as pl
from jax.experimental.pallas import tpu as pltpu
from jax.sharding import PartitionSpec as P

HEAD_SIZE = 128
KEYS = 256
SCALE = HEAD_SIZE**-0.5
SCALE2 = SCALE * 1.4426950408889634
MESH = pl.DeviceIdType.MESH
LANES = 128
norm_epsilon = 1e-06
rope_base = 1000000.0
loss_denominator = 16.0
masked_score = -1e30
VMEM = pl.BlockSpec(memory_space=pltpu.VMEM)
HBM = pl.BlockSpec(memory_space=pl.ANY)
dma = pltpu.SemaphoreType.DMA


def grid_of(count):
    across = 2 if count <= 16 else 4
    return count // (2 * across), across


def remote(src, dst, send, recv, where):
    return pltpu.make_async_remote_copy(
        src_ref=src, dst_ref=dst, send_sem=send, recv_sem=recv, device_id=where, device_id_type=MESH
    )


class Grid:
    def __init__(self, count, tower=False):
        self.lines, self.columns = grid_of(count)
        self.tower = tower
        self.across = 2 if tower else self.columns
        me, self.half = lax.axis_index("dp"), lax.axis_index("head")
        self.me = me
        self.core = me % 2
        self.column = (me // 2) % self.columns
        self.row = me // (2 * self.columns)
        self.col = self.half if tower else self.column

    def where(self, r, q, k):
        if self.tower:
            return {"dp": (r * self.columns + self.column) * 2 + k, "head": q}
        return {"dp": (r * self.columns + q) * 2 + k, "head": self.half}

    def index(self, r, q, k):
        return (r * self.across + q) * 2 + k


@dataclasses.dataclass
class Task:
    inputs: list
    in_specs: list
    outs: list
    out_specs: list
    scratch: list
    targets: Callable
    run: Callable
    pace: int = 1


def fuse(ident, name, *tasks):
    remote_ops = any(t.targets is not None for t in tasks)

    def split(refs, sizes):
        parts, start = [], 0
        for size in sizes:
            parts.append(refs[start : start + size])
            start += size
        return parts

    n_in = [len(t.inputs) for t in tasks]
    n_out = [len(t.outs) for t in tasks]
    n_scratch = [len(t.scratch) for t in tasks]

    def kernel(*refs):
        ins, outs, scratch = split(refs, [sum(n_in), sum(n_out), sum(n_scratch)])
        if remote_ops:
            barrier = pltpu.get_barrier_semaphore()
            known, total = set(), 0
            for t in tasks:
                for key, ok, where in t.targets() if t.targets is not None else ():
                    if key in known:
                        continue
                    known.add(key)
                    if ok is True:
                        pl.semaphore_signal(barrier, inc=1, device_id=where, device_id_type=MESH)
                        total = total + 1
                    else:

                        @pl.when(ok)
                        def _():
                            pl.semaphore_signal(barrier, inc=1, device_id=where, device_id_type=MESH)

                        total = total + ok.astype(jnp.int32)
            pl.semaphore_wait(barrier, total)
        live = [
            (t.run(*a, *b, *c), t.pace)
            for t, a, b, c in zip(tasks, split(ins, n_in), split(outs, n_out), split(scratch, n_scratch))
        ]
        while live:
            kept = []
            for steps, pace in live:
                for _ in range(pace):
                    if next(steps, None) is None:
                        break
                else:
                    kept.append((steps, pace))
            live = kept

    params = dict(vmem_limit_bytes=60 << 20)
    if remote_ops:
        params.update(collective_id=ident, has_side_effects=True)
    flat = pl.pallas_call(
        kernel,
        out_shape=[o for t in tasks for o in t.outs],
        in_specs=[s for t in tasks for s in t.in_specs],
        out_specs=[s for t in tasks for s in t.out_specs],
        scratch_shapes=[s for t in tasks for s in t.scratch],
        compiler_params=pltpu.CompilerParams(**params),
        name=name,
    )(*[x for t in tasks for x in t.inputs])
    return split(flat, n_out)


def gather(x, count, tower=False, pieces=1, both=False, pace=1):
    lines, columns = grid_of(count)
    across = 2 if tower else columns
    members = lines * across * 2
    shape = x.shape
    pieces = 1 if both else pieces
    x = x.reshape((pieces, shape[0] // pieces) + shape[1:])
    copies = 2 if both else pieces

    def hops_of(grid):
        row, col, core = grid.row, grid.col, grid.core
        return (
            (row < lines - 1, grid.where(row + 1, col, core)),
            (row > 0, grid.where(row - 1, col, core)),
            (col < across - 1, grid.where(row, col + 1, core)),
            (col > 0, grid.where(row, col - 1, core)),
            (True, grid.where(row, col, 1 - core)),
        )

    def targets():
        grid = Grid(count, tower)
        found = [(("hop", tower, i), ok, to) for i, (ok, to) in enumerate(hops_of(grid))]
        if both:
            found.append(("half", True, {"dp": grid.me, "head": 1 - grid.half}))
        return found

    def run(x_ref, o_ref, send, recv, local, cross):
        grid = Grid(count, tower)
        hops = hops_of(grid)
        core, col, row = grid.core, grid.col, grid.row
        me = grid.index(row, col, core)

        def copy(hop, shard, piece, src):
            return remote(src, o_ref.at[shard, piece], send.at[hop, shard, piece], recv.at[shard, piece], hops[hop][1])

        order = sorted(
            ((dr, dq) for dr in range(1 - lines, lines) for dq in range(1 - across, across)),
            key=lambda p: (abs(p[0]) + abs(p[1]), abs(p[1])),
        )
        if both:
            pair = remote(
                x_ref.at[0], o_ref.at[me, 1], cross.at[0], cross.at[1], {"dp": grid.me, "head": 1 - grid.half}
            )
            pair.start()
        sends = []
        mine = pltpu.make_async_copy(x_ref, o_ref.at[me, pl.ds(0, pieces)], local)
        for dr, dq in order:
            shard = grid.index(row - dr, col - dq, core)
            valid = (row - dr >= 0) & (row - dr < lines) & (col - dq >= 0) & (col - dq < across)
            onward = []
            if dq == 0:
                if dr >= 0:
                    onward.append(0)
                if dr <= 0:
                    onward.append(1)
            if dq >= 0:
                onward.append(2)
            if dq <= 0:
                onward.append(3)
            onward.append(4)
            for piece in range(copies):
                own = dr == 0 and dq == 0
                src = o_ref.at[shard, piece]
                if own and piece < pieces:
                    src = x_ref.at[piece]
                if own and piece >= pieces:
                    pair.wait_recv()
                if not own:

                    @pl.when(valid)
                    def _():
                        copy(4, shard, piece, src).wait_recv()

                for hop in onward:
                    ok = hops[hop][0]
                    go = valid if ok is True else valid & ok

                    @pl.when(go)
                    def _():
                        copy(hop, shard, piece, src).start()

                    sends.append((go, hop, shard, piece, src))
                yield True
            if dr == 0 and dq == 0:
                mine.start()
        for r in range(lines):
            for q in range(across):
                for piece in range(copies):
                    shard = grid.index(r, q, 1 - core)
                    copy(4, shard, piece, o_ref.at[shard, piece]).wait_recv()
        yield True
        for go, hop, shard, piece, src in sends:

            @pl.when(go)
            def _():
                copy(hop, shard, piece, src).wait_send()

        mine.wait()
        if both:
            pair.wait_send()

    return Task(
        [x],
        [VMEM],
        [jax.ShapeDtypeStruct((members, copies) + x.shape[1:], x.dtype)],
        [HBM],
        [dma((5, members, copies)), dma((members, copies)), dma, dma((2,))],
        targets,
        run,
        pace,
    )


def scatter(x, count, tower=False, dtype=jnp.float32, pace=1):
    lines, columns = grid_of(count)
    across = 2 if tower else columns
    members = lines * across * 2
    block = (x.shape[0] // members,) + x.shape[1:]
    height = block[0]
    step = 16
    x = x.reshape((members,) + block)

    def targets():
        grid = Grid(count, tower)
        row, col, core = grid.row, grid.col, grid.core
        found = [(("hop", tower, 4), True, grid.where(row, col, 1 - core))]
        found += [(("col", tower, e), True, grid.where(row, (col + e) % across, core)) for e in range(1, across)]
        found += [(("row", tower, d), True, grid.where((row + d) % lines, col, core)) for d in range(1, lines)]
        return found

    def run(x_ref, o_ref, near, first, wide, second, far, s1, r1, s2, r2, s3, r3):
        grid = Grid(count, tower)
        row, col, core = grid.row, grid.col, grid.core

        def one(r, q):
            return remote(
                x_ref.at[grid.index(r, q, 1 - core)], near.at[r, q], s1.at[r, q], r1.at[r, q], grid.where(row, col, 1 - core)
            )

        def two(r, e):
            return remote(
                first.at[r, e - 1], wide.at[r, e - 1], s2.at[r, e], r2.at[r, e], grid.where(row, (col + e) % across, core)
            )

        def three(d):
            return remote(
                second.at[d - 1], far.at[d - 1], s3.at[d], r3.at[d], grid.where((row + d) % lines, col, core)
            )

        lines_order = [d for d in range(1, lines)] + [0]
        for d in lines_order:
            r = (row + d) % lines
            for e in [e for e in range(1, across)] + [0]:
                one(r, (col + e) % across).start()
        yield True

        def blocks(body):
            def run_block(i, carry):
                body(pl.ds(pl.multiple_of(i * step, step), step))
                return carry

            lax.fori_loop(0, height // step, run_block, 0)

        for d in lines_order:
            r = (row + d) % lines
            for e in range(1, across):
                q = (col + e) % across
                one(r, q).wait_recv()

                def add(rows):
                    first[r, e - 1, rows] = (
                        x_ref[grid.index(r, q, core), rows].astype(jnp.float32) + near[r, q, rows].astype(jnp.float32)
                    ).astype(first.dtype)

                blocks(add)
                two(r, e).start()
            yield True
        for d in lines_order:
            r = (row + d) % lines
            one(r, col).wait_recv()
            for e in range(1, across):
                two(r, e).wait_recv()

            def total(rows):
                value = x_ref[grid.index(r, col, core), rows].astype(jnp.float32) + near[r, col, rows].astype(jnp.float32)
                for e in range(1, across):
                    value = value + wide[r, e - 1, rows].astype(jnp.float32)
                return value

            if d:

                def add(rows):
                    second[d - 1, rows] = total(rows).astype(second.dtype)

                blocks(add)
                three(d).start()
            else:
                for e in range(1, lines):
                    three(e).wait_recv()

                def add(rows):
                    value = total(rows)
                    for e in range(1, lines):
                        value = value + far[e - 1, rows].astype(jnp.float32)
                    o_ref[rows] = value.astype(o_ref.dtype)

                blocks(add)
            yield True
        for r in range(lines):
            for q in range(across):
                one(r, q).wait_send()
            for e in range(1, across):
                two(r, e).wait_send()
        for d in range(1, lines):
            three(d).wait_send()

    return Task(
        [x],
        [VMEM],
        [jax.ShapeDtypeStruct(block, dtype)],
        [VMEM],
        [
            pltpu.VMEM((lines, across) + block, x.dtype),
            pltpu.VMEM((lines, across - 1) + block, x.dtype),
            pltpu.VMEM((lines, across - 1) + block, x.dtype),
            pltpu.VMEM((lines - 1,) + block, x.dtype),
            pltpu.VMEM((lines - 1,) + block, x.dtype),
            dma((lines, across)),
            dma((lines, across)),
            dma((lines, across)),
            dma((lines, across)),
            dma((lines,)),
            dma((lines,)),
        ],
        targets,
        run,
        pace,
    )


def scatter_all(x, count, ident, name, **how):
    cuts = max(1, x.size * x.dtype.itemsize >> 23)
    span = x.shape[1] // cuts
    parts = [
        fuse(ident + i, f"{name}{i}", scatter(x[:, i * span : (i + 1) * span], count, **how))[0][0] for i in range(cuts)
    ]
    return parts[0] if cuts == 1 else jnp.concatenate(parts, axis=1)


def swap(arrays, pace=1):
    parts = len(arrays)

    def targets():
        return [("half", True, {"dp": lax.axis_index("dp"), "head": 1 - lax.axis_index("head")})]

    def run(*refs):
        ins, outs = refs[:parts], refs[parts : 2 * parts]
        send, recv = refs[2 * parts :]
        where = targets()[0][2]
        copies = [remote(ins[i], outs[i], send.at[i], recv.at[i], where) for i in range(parts)]
        for copy in copies:
            copy.start()
        yield True
        for copy in copies:
            copy.wait()

    return Task(
        list(arrays),
        [VMEM] * parts,
        [jax.ShapeDtypeStruct(a.shape, a.dtype) for a in arrays],
        [VMEM] * parts,
        [dma((parts,)), dma((parts,))],
        targets,
        run,
        pace,
    )


def unit_targets(count):
    lines, columns = grid_of(count)
    grid = Grid(count)
    mine = grid.row * 2 + grid.core
    found = []
    for e in range(1, 2 * lines):
        member = mine ^ e
        found.append((("member", e), True, grid.where(member // 2, grid.column, member % 2)))
    for e in range(1, columns):
        found.append((("col", False, e), True, grid.where(grid.row, (grid.column + e) % columns, grid.core)))
    return found


def spread(w, count, pace=1):
    lines, columns = grid_of(count)
    kinds, depth, width = w.shape
    tiles = width // LANES
    members = 2 * lines
    slots = pl.cdiv(tiles, members)
    twice = 2 * depth

    def run(w_ref, o_ref, zeros, send, recv, push, pull, blank):
        grid = Grid(count)
        mine = grid.row * 2 + grid.core

        def lanes(slot):
            return pl.ds(slot * LANES, LANES)

        def bytes_of(slot):
            return o_ref.at[:, pl.ds(0, members * depth), lanes(slot)]

        def full(slot, member):
            return True if (slot + 1) * members <= tiles else slot * members + member < tiles

        def guarded(ok, body):
            if ok is True:
                body()
            else:
                pl.when(ok)(body)

        def block(slot, member):
            return w_ref.at[:, :, pl.ds(pl.multiple_of((slot * members + member) * LANES, LANES), LANES)]

        def spot(slot):
            return o_ref.at[:, pl.ds(pl.multiple_of(grid.me * depth, depth), depth), lanes(slot)]

        def out(slot, e):
            member = mine ^ e
            return remote(
                block(slot, member),
                spot(slot),
                send.at[slot, e],
                recv.at[slot],
                grid.where(member // 2, grid.column, member % 2),
            )

        def chunk(slot, r, column):
            return o_ref.at[:, pl.ds(pl.multiple_of((r * columns + column) * twice, twice), twice), lanes(slot)]

        def over(slot, r, e):
            here = chunk(slot, r, grid.column)
            return remote(
                here,
                here,
                push.at[slot, r, e],
                pull.at[slot, e],
                grid.where(grid.row, (grid.column + e) % columns, grid.core),
            )

        for slot in range(slots):
            for e in range(1, members):
                guarded(full(slot, mine ^ e), lambda: out(slot, e).start())
            guarded(
                full(slot, mine), lambda: pltpu.make_async_copy(block(slot, mine), spot(slot), recv.at[slot]).start()
            )
        last = slots - 1
        some = full(last, mine)
        if some is not True:
            fills = [
                pltpu.make_async_copy(zeros, o_ref.at[:, pl.ds(i * depth, depth), lanes(last)], blank.at[i])
                for i in range(count)
            ]

            @pl.when(jnp.logical_not(some))
            def _():
                zeros[...] = jnp.zeros_like(zeros)
                for fill in fills:
                    fill.start()
                for fill in fills:
                    fill.wait()

        yield True
        for slot in range(slots):

            def pass_on():
                pltpu.make_async_copy(bytes_of(slot), bytes_of(slot), recv.at[slot]).wait()
                for r in range(lines):
                    for e in range(1, columns):
                        over(slot, r, e).start()

            guarded(full(slot, mine), pass_on)
            yield True
        for slot in range(slots):

            def finish():
                for e in range(1, columns):
                    pltpu.make_async_copy(bytes_of(slot), bytes_of(slot), pull.at[slot, e]).wait()
                    for r in range(lines):
                        over(slot, r, e).wait_send()

            guarded(full(slot, mine), finish)
            for e in range(1, members):
                guarded(full(slot, mine ^ e), lambda: out(slot, e).wait_send())

    return Task(
        [w],
        [VMEM],
        [jax.ShapeDtypeStruct((kinds, count * depth, slots * LANES), w.dtype)],
        [HBM],
        [
            pltpu.VMEM((kinds, depth, LANES), w.dtype),
            dma((slots, members)),
            dma((slots,)),
            dma((slots, lines, columns)),
            dma((slots, columns)),
            dma((count,)),
        ],
        functools.partial(unit_targets, count),
        run,
        pace,
    )


def collect(g, count, width, pace=1):
    lines, columns = grid_of(count)
    kinds, rows, span = g.shape
    tiles = width // LANES
    members = 2 * lines
    slots = span // LANES
    depth = rows // count
    twice = 2 * depth

    def run(g_ref, o_ref, near, stage, push, pull, send, recv):
        grid = Grid(count)
        mine = grid.row * 2 + grid.core

        def lanes(slot):
            return pl.ds(slot * LANES, LANES)

        def guarded(slot, body):
            if (slot + 1) * members <= tiles:
                body()
            else:
                pl.when(slot * members + mine < tiles)(body)

        def rows_at(r, column):
            return pl.multiple_of((r * columns + column) * twice, twice)

        def over(slot, r, e):
            column = (grid.column + e) % columns
            return remote(
                g_ref.at[:, pl.ds(rows_at(r, column), twice), lanes(slot)],
                near.at[slot, e - 1, :, pl.ds(r * twice, twice)],
                push.at[slot, r, e],
                pull.at[slot, e],
                grid.where(grid.row, column, grid.core),
            )

        def spot(slot):
            return o_ref.at[:, :, pl.ds(pl.multiple_of((slot * members + mine) * LANES, LANES), LANES)]

        def piece(slot, member):
            return stage.at[slot, :, pl.ds(pl.multiple_of(member * depth, depth), depth)]

        def out(slot, e):
            member = mine ^ e
            return remote(
                piece(slot, member),
                spot(slot),
                send.at[slot, e],
                recv,
                grid.where(member // 2, grid.column, member % 2),
            )

        for slot in range(slots):

            def begin():
                for e in range(1, columns):
                    for r in range(lines):
                        over(slot, r, e).start()

            guarded(slot, begin)
        yield True
        for slot in range(slots):

            def add_up():
                for e in range(1, columns):
                    pltpu.make_async_copy(near.at[slot, e - 1], near.at[slot, e - 1], pull.at[slot, e]).wait()

                def add(i, carry):
                    for r in range(lines):
                        here = pl.ds(pl.multiple_of(rows_at(r, grid.column) + i * 16, 16), 16)
                        there = pl.ds(pl.multiple_of(r * twice + i * 16, 16), 16)
                        for kind in range(kinds):
                            value = g_ref[kind, here, lanes(slot)].astype(jnp.float32)
                            for e in range(1, columns):
                                value = value + near[slot, e - 1, kind, there].astype(jnp.float32)
                            stage[slot, kind, there] = value.astype(stage.dtype)
                    return carry

                lax.fori_loop(0, twice // 16, add, 0)
                for e in range(1, members):
                    out(slot, e).start()
                pltpu.make_async_copy(piece(slot, mine), spot(slot), recv).start()

            guarded(slot, add_up)
            yield True
        pltpu.make_async_copy(o_ref, o_ref, recv).wait()
        for slot in range(slots):

            def finish():
                for e in range(1, columns):
                    for r in range(lines):
                        over(slot, r, e).wait_send()
                for e in range(1, members):
                    out(slot, e).wait_send()

            guarded(slot, finish)

    return Task(
        [g],
        [VMEM],
        [jax.ShapeDtypeStruct((kinds, depth, width), g.dtype)],
        [VMEM],
        [
            pltpu.VMEM((slots, columns - 1, kinds, members * depth, LANES), g.dtype),
            pltpu.VMEM((slots, kinds, members * depth, LANES), g.dtype),
            dma((slots, lines, columns)),
            dma((slots, columns)),
            dma((slots, members)),
            dma,
        ],
        functools.partial(unit_targets, count),
        run,
        pace,
    )


def window(most):
    def bounds(tokens):
        first = lax.axis_index("dp") * tokens
        return jnp.maximum(first - most + 1, 0) // KEYS, (first + tokens - 1) // KEYS + 1, first

    return bounds


def attend(most, begin, q, kv, pace=1):
    tokens, heads = q.shape[0], q.shape[1] // HEAD_SIZE

    def run(begin_ref, q_ref, kv_ref, o_ref, lse_ref):
        low, high, first = window(most)(tokens)
        begin = begin_ref[...]
        index = first + lax.broadcasted_iota(jnp.int32, (tokens, 1), 0)
        lane = lax.broadcasted_iota(jnp.int32, (tokens, HEAD_SIZE), 1)
        key_lane = lax.broadcasted_iota(jnp.int32, (tokens, KEYS), 1)
        yield True
        for h in range(heads):
            cols = slice(h * HEAD_SIZE, (h + 1) * HEAD_SIZE)

            def step(block, state):
                top, mass, total = state
                start = pl.multiple_of(block * KEYS, KEYS)
                keys = kv_ref[pl.ds(start, KEYS), :HEAD_SIZE]
                values = kv_ref[pl.ds(start, KEYS), HEAD_SIZE:]
                scores = lax.dot_general(
                    q_ref[:, cols], keys, (((1,), (1,)), ((), ())), preferred_element_type=jnp.float32
                )
                at = key_lane + start
                scores = jnp.where((at >= begin) & (at <= index), scores * SCALE2, masked_score)
                best = jnp.maximum(top, jnp.max(scores, axis=1, keepdims=True))
                fade = jnp.exp2(top - best)
                probs = jnp.exp2(scores - best)
                mass = mass * fade + jnp.sum(probs, axis=1, keepdims=True)
                total = total * fade + jnp.dot(
                    probs.astype(jnp.bfloat16), values, preferred_element_type=jnp.float32
                )
                return best, mass, total

            top, mass, total = lax.fori_loop(
                low,
                high,
                step,
                (
                    jnp.full((tokens, 1), masked_score, jnp.float32),
                    jnp.zeros((tokens, 1), jnp.float32),
                    jnp.zeros((tokens, HEAD_SIZE), jnp.float32),
                ),
            )
            o_ref[:, cols] = total / mass
            lse = top + jnp.log2(mass)
            lse_ref[...] = jnp.where(lane == h, lse, 0.0 if h == 0 else lse_ref[...])
            yield True

    return Task(
        [begin, q, kv],
        [VMEM] * 3,
        [jax.ShapeDtypeStruct(q.shape, jnp.float32), jax.ShapeDtypeStruct((tokens, HEAD_SIZE), jnp.float32)],
        [VMEM] * 2,
        [],
        None,
        run,
        pace,
    )


def attend_back(most, begin, q, kv, lse, raw, do, pace=1):
    tokens, heads = q.shape[0], q.shape[1] // HEAD_SIZE
    across = (((1,), (1,)), ((), ()))
    down = (((0,), (0,)), ((), ()))

    def run(begin_ref, q_ref, kv_ref, lse_ref, raw_ref, do_ref, dq_ref, dkv_ref, delta_ref):
        low, high, first = window(most)(tokens)
        begin = begin_ref[...]
        index = first + lax.broadcasted_iota(jnp.int32, (tokens, 1), 0)
        lane = lax.broadcasted_iota(jnp.int32, (tokens, HEAD_SIZE), 1)
        key_lane = lax.broadcasted_iota(jnp.int32, (tokens, KEYS), 1)
        table = jnp.zeros((tokens, HEAD_SIZE), jnp.float32)
        for h in range(heads):
            cols = slice(h * HEAD_SIZE, (h + 1) * HEAD_SIZE)
            delta = jnp.sum(do_ref[:, cols].astype(jnp.float32) * raw_ref[:, cols], axis=1, keepdims=True)
            table = jnp.where(lane == h, delta, table)
        delta_ref[...] = table
        dq_ref[...] = jnp.zeros_like(dq_ref)
        blocks = kv_ref.shape[0] // KEYS

        def clear(block, carry):
            rows = pl.ds(pl.multiple_of(block * KEYS, KEYS), KEYS)
            dkv_ref[rows, :] = jnp.zeros((KEYS, 2 * HEAD_SIZE), dkv_ref.dtype)
            return carry

        lax.fori_loop(0, low, clear, 0)
        lax.fori_loop(high, blocks, clear, 0)

        def step(block, carry):
            start = pl.multiple_of(block * KEYS, KEYS)
            rows = pl.ds(start, KEYS)
            keys = kv_ref[rows, :HEAD_SIZE]
            values = kv_ref[rows, HEAD_SIZE:]
            at = key_lane + start
            seen = (at >= begin) & (at <= index)
            dk = jnp.zeros((KEYS, HEAD_SIZE), jnp.float32)
            dv = jnp.zeros((KEYS, HEAD_SIZE), jnp.float32)
            for h in range(heads):
                cols = slice(h * HEAD_SIZE, (h + 1) * HEAD_SIZE)
                q = q_ref[:, cols]
                do = do_ref[:, cols]
                scores = lax.dot_general(q, keys, across, preferred_element_type=jnp.float32)
                probs = jnp.where(seen, jnp.exp2(scores * SCALE2 - lse_ref[:, h : h + 1]), 0.0)
                pull = lax.dot_general(do, values, across, preferred_element_type=jnp.float32)
                ds = (probs * (pull - delta_ref[:, h : h + 1])).astype(jnp.bfloat16)
                dq_ref[:, cols] += jnp.dot(ds, keys, preferred_element_type=jnp.float32)
                dk = dk + lax.dot_general(ds, q, down, preferred_element_type=jnp.float32)
                dv = dv + lax.dot_general(
                    probs.astype(jnp.bfloat16), do, down, preferred_element_type=jnp.float32
                )
            dkv_ref[rows, :HEAD_SIZE] = (dk * SCALE).astype(dkv_ref.dtype)
            dkv_ref[rows, HEAD_SIZE:] = dv.astype(dkv_ref.dtype)
            return carry

        parts = 3
        reach = high - low
        yield True
        for i in range(parts):
            lax.fori_loop(low + reach * i // parts, low + reach * (i + 1) // parts, step, 0)
            yield True

    return Task(
        [begin, q, kv, lse, raw, do],
        [VMEM] * 6,
        [jax.ShapeDtypeStruct(q.shape, jnp.float32), jax.ShapeDtypeStruct(kv.shape, kv.dtype)],
        [VMEM] * 2,
        [pltpu.VMEM((tokens, HEAD_SIZE), jnp.float32)],
        None,
        run,
        pace,
    )


def doc_layout(row_lengths, first_token, token_count):
    doc_ends = jnp.cumsum(row_lengths)
    doc_starts = doc_ends - row_lengths
    token_index = first_token + jnp.arange(token_count, dtype=jnp.int32)
    doc_begin = jnp.max(
        jnp.where(doc_starts[None, :] <= token_index[:, None], doc_starts[None, :], 0), axis=1
    )
    return (doc_begin, token_index - doc_begin)


def rope_tables(positions):
    freq = rope_base ** (-jnp.arange(0, HEAD_SIZE, 2, dtype=jnp.float32) / HEAD_SIZE)
    angle = positions.astype(jnp.float32)[:, None] * freq[None, :]
    angle = jnp.concatenate([angle, angle], axis=1)
    return (jnp.cos(angle)[:, None, :], jnp.sin(angle)[:, None, :])


def rotary_apply(values, cosine_table, sine_table):
    half_width = values.shape[-1] // 2
    turned = jnp.concatenate([-values[..., half_width:], values[..., :half_width]], axis=-1)
    return values * cosine_table + turned * sine_table


def unrotate(grads, cosine_table, sine_table):
    half_width = grads.shape[-1] // 2
    scaled_grad = grads * sine_table
    back_part = jnp.concatenate(
        [scaled_grad[..., half_width:], -scaled_grad[..., :half_width]], axis=-1
    )
    return grads * cosine_table + back_part


def rms_scale(values):
    return lax.rsqrt(jnp.mean(values * values, axis=-1, keepdims=True) + norm_epsilon)


def norm_back(grad_out, inputs, scale, gain):
    weighted = grad_out * gain
    return scale * weighted - inputs * scale**3 * jnp.mean(
        weighted * inputs, axis=-1, keepdims=True
    )


def dot(a, b, dims=((1,), (0,))):
    return lax.dot_general(a, b, (dims, ((), ())), preferred_element_type=jnp.float32)


across_dims = ((1,), (1,))
token_dims = ((0,), (0,))


def longest(token_count):
    return 2048 if token_count == 4096 else token_count


def body(
    count,
    layer_in,
    gain_attn,
    q_weight,
    q_bias,
    key_weight,
    key_bias,
    value_weight,
    value_bias,
    o_weight,
    gain_mlp,
    gate_weight,
    up_weight,
    down_weight,
    row_lengths,
    source_ids,
    source_weights,
    out_grad,
):
    f32, bf16 = jnp.float32, jnp.bfloat16
    tok_rows, width = layer_in.shape
    part = tok_rows // 2
    half = lax.axis_index("head")
    first_token = lax.axis_index("dp") * tok_rows
    doc_begin, positions = doc_layout(row_lengths, first_token, tok_rows)
    cosine_table, sine_table = rope_tables(positions)
    q_cols = q_weight.shape[1]
    kv_cols = key_weight.shape[1]
    heads = q_cols // HEAD_SIZE
    ff_cols = gate_weight.shape[1]

    def mine(rows):
        return lax.dynamic_slice_in_dim(rows, half * part, part, 0)

    def other(rows):
        return lax.dynamic_slice_in_dim(rows, (1 - half) * part, part, 0)

    def join(own, peer):
        return jnp.where(half == 0, jnp.concatenate([own, peer]), jnp.concatenate([peer, own]))

    attn_local = jnp.concatenate([q_weight, key_weight, value_weight, o_weight.T], axis=1)
    picked = source_ids[:, None] == jnp.arange(source_weights.shape[0], dtype=jnp.int32)[None, :]
    row_scale = (
        jnp.sum(jnp.where(picked, source_weights[None, :], 0), axis=1).astype(f32) / loss_denominator
    )
    cotangent = mine(out_grad).astype(f32) * mine(row_scale[:, None])
    ((attn_full,), (grad_all,)) = fuse(
        1, "gather_inputs", gather(attn_local, count), gather(cotangent.astype(bf16), count, tower=True)
    )
    attn_full = attn_full.reshape(width, -1)
    grad_all = grad_all.reshape(-1, width)
    qkv_cols = q_cols + 2 * kv_cols
    full_qkv = attn_full[:, :qkv_cols]
    full_o = attn_full[:, qkv_cols:]
    inputs = layer_in.astype(f32)
    scale_one = rms_scale(inputs)
    gain_one = gain_attn.astype(f32)
    normed = (inputs * scale_one * gain_one).astype(bf16)
    bias = jnp.concatenate([q_bias, key_bias, value_bias]).astype(f32)
    pre = dot(normed, full_qkv) + bias
    turned = rotary_apply(
        pre[:, : q_cols + kv_cols].reshape(tok_rows, heads + 1, HEAD_SIZE), cosine_table, sine_table
    ).reshape(tok_rows, q_cols + kv_cols)
    query_rows = turned[:, :q_cols].astype(bf16)
    kv_rows = jnp.concatenate([turned[:, q_cols:], pre[:, q_cols + kv_cols :]], axis=1).astype(bf16)
    ((kv_all,),) = fuse(2, "gather_keys", gather(kv_rows, count))
    kv_all = kv_all.reshape(-1, 2 * kv_cols)
    begin = doc_begin[:, None].astype(jnp.int32)
    most = longest(count * tok_rows)
    mlp_local = jnp.stack([gate_weight, up_weight, down_weight.T])
    ((attended_raw, row_lse), (mlp_full,)) = fuse(
        3, "attend_spread", attend(most, begin, query_rows, kv_all), spread(mlp_local, count)
    )
    attended = attended_raw.astype(bf16)
    branch_part = dot(attended, full_o, across_dims)
    ((branch_peer,),) = fuse(4, "swap_branch", swap([other(branch_part).astype(bf16)]))
    hidden = mine(inputs) + (mine(branch_part) + branch_peer.astype(f32))
    scale_two = rms_scale(hidden)
    gain_two = gain_mlp.astype(f32)
    normed_mlp = (hidden * scale_two * gain_two).astype(bf16)
    ((rows_all,),) = fuse(5, "gather_rows", gather(normed_mlp, count, tower=True))
    rows_all = rows_all.reshape(-1, width)

    full_gate, full_up, full_down = mlp_full[0], mlp_full[1], mlp_full[2]
    gate_act = dot(rows_all, full_gate)
    up_act = dot(rows_all, full_up)
    sigmoid_gate = jax.nn.sigmoid(gate_act)
    silu_gate = gate_act * sigmoid_gate
    active = (silu_gate * up_act).astype(bf16)
    d_active = dot(grad_all, full_down)
    d_gate = (d_active * up_act * sigmoid_gate * (1.0 + gate_act * (1.0 - sigmoid_gate))).astype(bf16)
    d_up = (d_active * silu_gate).astype(bf16)
    mlp_part = dot(active, full_down, across_dims).astype(bf16)
    norm_two_part = (dot(d_gate, full_gate, across_dims) + dot(d_up, full_up, across_dims)).astype(bf16)
    mlp_grads = jnp.stack(
        [
            dot(rows_all, d_gate, token_dims).astype(bf16),
            dot(rows_all, d_up, token_dims).astype(bf16),
            dot(grad_all, active, token_dims).astype(bf16),
        ]
    )
    d_normed_mlp = scatter_all(norm_two_part, count, 8, "scatter_rows", tower=True)
    gain_two_local = jnp.sum(d_normed_mlp * hidden * scale_two, axis=0)
    d_hidden = cotangent + norm_back(d_normed_mlp, hidden, scale_two, gain_two)
    branch_own = d_hidden.astype(bf16)
    ((branch_peer,),) = fuse(16, "swap_grad", swap([branch_own]))
    branch_grad = join(branch_own, branch_peer)
    out_proj_grad = dot(branch_grad, attended, token_dims)
    d_attended = dot(branch_grad, full_o).astype(bf16)
    ((d_query, d_kv), (mlp_part_sums,)) = fuse(
        17,
        "attend_back_collect",
        attend_back(most, begin, query_rows, kv_all, row_lse, attended_raw, d_attended),
        collect(mlp_grads, count, ff_cols),
    )
    mlp_part_sums = mlp_part_sums.astype(f32)
    kv_sums = scatter_all(d_kv, count, 18, "scatter_keys")
    d_queries = (d_query * SCALE).astype(bf16).astype(f32)
    d_key_rot = kv_sums[:, :kv_cols].astype(bf16).astype(f32)
    d_value_rows = kv_sums[:, kv_cols:].astype(bf16)
    d_turned = jnp.concatenate([d_queries, d_key_rot], axis=1).reshape(tok_rows, heads + 1, HEAD_SIZE)
    d_pre = jnp.concatenate(
        [
            unrotate(d_turned, cosine_table, sine_table).reshape(tok_rows, q_cols + kv_cols).astype(bf16),
            d_value_rows,
        ],
        axis=1,
    )
    bias_local = jnp.sum(d_pre.astype(f32), axis=0)
    qkv_grad = dot(normed, d_pre, token_dims)
    attn_grads = jnp.concatenate([qkv_grad, out_proj_grad], axis=1).astype(bf16)
    norm_one_part = dot(d_pre, full_qkv, across_dims)
    norm_send = other(norm_one_part).astype(bf16)
    if count <= 16:
        ((attn_part,), (mlp_out,), (norm_peer,)) = fuse(
            21, "scatter_last", scatter(attn_grads, count), scatter(mlp_part, count, tower=True), swap([norm_send])
        )
    else:
        attn_part = scatter_all(attn_grads, count, 21, "scatter_attn")
        mlp_out = scatter_all(mlp_part, count, 25, "scatter_out", tower=True)
        ((norm_peer,),) = fuse(33, "swap_norm", swap([norm_send]))
    layer_out_own = (hidden + mlp_out).astype(bf16)
    d_normed = mine(norm_one_part) + norm_peer.astype(f32)
    inputs_own = mine(inputs)
    scale_own = mine(scale_one)
    gain_one_local = jnp.sum(d_normed * inputs_own * scale_own, axis=0)
    layer_in_grad_own = (d_hidden + norm_back(d_normed, inputs_own, scale_own, gain_one)).astype(bf16)

    small = jnp.concatenate([bias_local, gain_one_local, gain_two_local]).reshape(-1, LANES)
    ((small_all,), (layer_in_grad_peer, layer_out_peer)) = fuse(
        34, "gather_sums", gather(small, count, both=True), swap([layer_in_grad_own, layer_out_own])
    )
    small_all = small_all.reshape(count, 2, -1)
    small_sum = jnp.sum(small_all[:, 0], axis=0)
    gains = (small_sum[qkv_cols:] + jnp.sum(small_all[:, 1, qkv_cols:], axis=0)).reshape(2, width)
    layer_in_grad = join(layer_in_grad_own, layer_in_grad_peer)
    layer_out = join(layer_out_own, layer_out_peer)
    return (
        layer_out,
        layer_in_grad,
        gains[0],
        attn_part[:, :q_cols],
        small_sum[:q_cols],
        attn_part[:, q_cols : q_cols + kv_cols],
        small_sum[q_cols : q_cols + kv_cols],
        attn_part[:, q_cols + kv_cols : qkv_cols],
        small_sum[q_cols + kv_cols : qkv_cols],
        attn_part[:, qkv_cols:].T,
        gains[1],
        mlp_part_sums[0],
        mlp_part_sums[1],
        mlp_part_sums[2].T,
    )


def solution(mesh):
    placed = (
        P("dp", None),
        P(),
        P("dp", "head"),
        P("head"),
        P("dp", "head"),
        P("head"),
        P("dp", "head"),
        P("head"),
        P("head", "dp"),
        P(),
        P("dp", "head"),
        P("dp", "head"),
        P("head", "dp"),
        P(),
        P("dp"),
        P(),
        P("dp", None),
    )
    return jax.shard_map(
        functools.partial(body, mesh.shape["dp"]),
        mesh=mesh,
        in_specs=placed,
        out_specs=(
            P("dp", None),
            P("dp", None),
            P(),
            P("dp", "head"),
            P("head"),
            P("dp", "head"),
            P("head"),
            P("dp", "head"),
            P("head"),
            P("head", "dp"),
            P(),
            P("dp", "head"),
            P("dp", "head"),
            P("head", "dp"),
        ),
        check_vma=False,
    )
```

```python
import dataclasses
import functools
from typing import Any, Callable
import jax
import jax.numpy as jnp
from jax import lax
from jax.experimental import pallas as pl
from jax.experimental.pallas import tpu as pltpu
from jax.sharding import PartitionSpec as P

HEAD_SIZE = 128
KEYS = 256
SCALE = HEAD_SIZE**-0.5
SCALE2 = SCALE * 1.4426950408889634
MESH = pl.DeviceIdType.MESH
LANES = 128
norm_epsilon = 1e-06
rope_base = 1000000.0
loss_denominator = 16.0
masked_score = -1e30
VMEM = pl.BlockSpec(memory_space=pltpu.VMEM)
HBM = pl.BlockSpec(memory_space=pl.ANY)
dma = pltpu.SemaphoreType.DMA


def grid_of(count):
    across = 2 if count <= 16 else 4
    return count // (2 * across), across


def remote(src, dst, send, recv, where):
    return pltpu.make_async_remote_copy(
        src_ref=src, dst_ref=dst, send_sem=send, recv_sem=recv, device_id=where, device_id_type=MESH
    )


def reshape(x, shape):
    if isinstance(x, jax.ShapeDtypeStruct):
        return jax.ShapeDtypeStruct(shape, x.dtype)
    return x.reshape(shape)


class Grid:
    def __init__(self, count, tower=False):
        self.lines, self.columns = grid_of(count)
        self.tower = tower
        self.across = 2 if tower else self.columns
        me, self.half = lax.axis_index("dp"), lax.axis_index("head")
        self.me = me
        self.core = me % 2
        self.column = (me // 2) % self.columns
        self.row = me // (2 * self.columns)
        self.col = self.half if tower else self.column

    def where(self, r, q, k):
        if self.tower:
            return {"dp": (r * self.columns + self.column) * 2 + k, "head": q}
        return {"dp": (r * self.columns + q) * 2 + k, "head": self.half}

    def index(self, r, q, k):
        return (r * self.across + q) * 2 + k


@dataclasses.dataclass
class Task:
    inputs: list
    in_specs: list
    outs: list
    out_specs: list
    scratch: list
    targets: Callable
    run: Callable


def fuse(ident, name, *tasks, order=()):
    remote_ops = any(t.targets is not None for t in tasks)

    def split(refs, sizes):
        parts, start = [], 0
        for size in sizes:
            parts.append(refs[start : start + size])
            start += size
        return parts

    n_in = [len(t.inputs) for t in tasks]
    n_out = [len(t.outs) for t in tasks]
    n_scratch = [len(t.scratch) for t in tasks]

    def kernel(*refs):
        ins, outs, scratch = split(refs, [sum(n_in), sum(n_out), sum(n_scratch)])
        if remote_ops:
            barrier = pltpu.get_barrier_semaphore()
            known, total = set(), 0
            for t in tasks:
                for key, ok, where in t.targets() if t.targets is not None else ():
                    if key in known:
                        continue
                    known.add(key)
                    if ok is True:
                        pl.semaphore_signal(barrier, inc=1, device_id=where, device_id_type=MESH)
                        total = total + 1
                    else:

                        @pl.when(ok)
                        def _():
                            pl.semaphore_signal(barrier, inc=1, device_id=where, device_id_type=MESH)

                        total = total + ok.astype(jnp.int32)
            pl.semaphore_wait(barrier, total)
        steps = [
            t.run(*a, *b, *c)
            for t, a, b, c in zip(tasks, split(ins, n_in), split(outs, n_out), split(scratch, n_scratch))
        ]
        live = set(range(len(steps)))
        turns = list(order)
        while live:
            for i in turns:
                if i in live and next(steps[i], None) is None:
                    live.remove(i)
            turns = sorted(live)

    params = dict(vmem_limit_bytes=60 << 20)
    if remote_ops:
        params.update(collective_id=ident, has_side_effects=True)
    flat = pl.pallas_call(
        kernel,
        out_shape=[o for t in tasks for o in t.outs],
        in_specs=[s for t in tasks for s in t.in_specs],
        out_specs=[s for t in tasks for s in t.out_specs],
        scratch_shapes=[s for t in tasks for s in t.scratch],
        compiler_params=pltpu.CompilerParams(**params),
        name=name,
    )(*[x for t in tasks for x in t.inputs])
    return split(flat, n_out)


def gather(x, count, tower=False, pieces=1, both=False):
    lines, columns = grid_of(count)
    across = 2 if tower else columns
    members = lines * across * 2
    shape = x.shape
    pieces = 1 if both else pieces
    x = reshape(x, (pieces, shape[0] // pieces) + shape[1:])
    copies = 2 if both else pieces

    def hops_of(grid):
        row, col, core = grid.row, grid.col, grid.core
        return (
            (row < lines - 1, grid.where(row + 1, col, core)),
            (row > 0, grid.where(row - 1, col, core)),
            (col < across - 1, grid.where(row, col + 1, core)),
            (col > 0, grid.where(row, col - 1, core)),
            (True, grid.where(row, col, 1 - core)),
        )

    def targets():
        grid = Grid(count, tower)
        found = [(("hop", tower, i), ok, to) for i, (ok, to) in enumerate(hops_of(grid))]
        if both:
            found.append(("half", True, {"dp": grid.me, "head": 1 - grid.half}))
        return found

    def run(x_ref, o_ref, send, recv, local, cross):
        grid = Grid(count, tower)
        hops = hops_of(grid)
        core, col, row = grid.core, grid.col, grid.row
        me = grid.index(row, col, core)

        def copy(hop, shard, piece, src):
            return remote(src, o_ref.at[shard, piece], send.at[hop, shard, piece], recv.at[shard, piece], hops[hop][1])

        order = sorted(
            ((dr, dq) for dr in range(1 - lines, lines) for dq in range(1 - across, across)),
            key=lambda p: (abs(p[0]) + abs(p[1]), abs(p[1])),
        )
        if both:
            pair = remote(
                x_ref.at[0], o_ref.at[me, 1], cross.at[0], cross.at[1], {"dp": grid.me, "head": 1 - grid.half}
            )
            pair.start()
        sends = []
        mine = pltpu.make_async_copy(x_ref, o_ref.at[me, pl.ds(0, pieces)], local)
        for dr, dq in order:
            shard = grid.index(row - dr, col - dq, core)
            valid = (row - dr >= 0) & (row - dr < lines) & (col - dq >= 0) & (col - dq < across)
            onward = []
            if dq == 0:
                if dr >= 0:
                    onward.append(0)
                if dr <= 0:
                    onward.append(1)
            if dq >= 0:
                onward.append(2)
            if dq <= 0:
                onward.append(3)
            onward.append(4)
            for piece in range(copies):
                own = dr == 0 and dq == 0
                src = o_ref.at[shard, piece]
                if own and piece < pieces:
                    src = x_ref.at[piece]
                if own and piece >= pieces:
                    pair.wait_recv()
                if not own:

                    @pl.when(valid)
                    def _():
                        copy(4, shard, piece, src).wait_recv()

                for hop in onward:
                    ok = hops[hop][0]
                    go = valid if ok is True else valid & ok

                    @pl.when(go)
                    def _():
                        copy(hop, shard, piece, src).start()

                    sends.append((go, hop, shard, piece, src))
                yield True
            if dr == 0 and dq == 0:
                mine.start()
        for r in range(lines):
            for q in range(across):
                for piece in range(copies):
                    shard = grid.index(r, q, 1 - core)
                    copy(4, shard, piece, o_ref.at[shard, piece]).wait_recv()
        yield True
        for go, hop, shard, piece, src in sends:

            @pl.when(go)
            def _():
                copy(hop, shard, piece, src).wait_send()

        mine.wait()
        if both:
            pair.wait_send()

    return Task(
        [x],
        [VMEM],
        [jax.ShapeDtypeStruct((members, copies) + x.shape[1:], x.dtype)],
        [HBM],
        [dma((5, members, copies)), dma((members, copies)), dma, dma((2,))],
        targets,
        run,
    )


def scatter(x, count, tower=False, dtype=jnp.float32):
    lines, columns = grid_of(count)
    across = 2 if tower else columns
    members = lines * across * 2
    block = (x.shape[0] // members,) + x.shape[1:]
    height = block[0]
    step = 16
    x = reshape(x, (members,) + block)

    def targets():
        grid = Grid(count, tower)
        row, col, core = grid.row, grid.col, grid.core
        found = [(("hop", tower, 4), True, grid.where(row, col, 1 - core))]
        found += [(("col", tower, e), True, grid.where(row, (col + e) % across, core)) for e in range(1, across)]
        found += [(("row", tower, d), True, grid.where((row + d) % lines, col, core)) for d in range(1, lines)]
        return found

    def run(x_ref, o_ref, near, first, wide, second, far, s1, r1, s2, r2, s3, r3):
        grid = Grid(count, tower)
        row, col, core = grid.row, grid.col, grid.core

        def one(r, q):
            return remote(
                x_ref.at[grid.index(r, q, 1 - core)], near.at[r, q], s1.at[r, q], r1.at[r, q], grid.where(row, col, 1 - core)
            )

        def two(r, e):
            return remote(
                first.at[r, e - 1], wide.at[r, e - 1], s2.at[r, e], r2.at[r, e], grid.where(row, (col + e) % across, core)
            )

        def three(d):
            return remote(
                second.at[d - 1], far.at[d - 1], s3.at[d], r3.at[d], grid.where((row + d) % lines, col, core)
            )

        lines_order = [d for d in range(1, lines)] + [0]
        for d in lines_order:
            r = (row + d) % lines
            for e in [e for e in range(1, across)] + [0]:
                one(r, (col + e) % across).start()
        yield True

        def blocks(body):
            def run_block(i, carry):
                body(pl.ds(pl.multiple_of(i * step, step), step))
                return carry

            lax.fori_loop(0, height // step, run_block, 0)

        for d in lines_order:
            r = (row + d) % lines
            for e in range(1, across):
                q = (col + e) % across
                one(r, q).wait_recv()

                def add(rows):
                    first[r, e - 1, rows] = (
                        x_ref[grid.index(r, q, core), rows].astype(jnp.float32) + near[r, q, rows].astype(jnp.float32)
                    ).astype(first.dtype)

                blocks(add)
                two(r, e).start()
            yield True
        for d in lines_order:
            r = (row + d) % lines
            one(r, col).wait_recv()
            for e in range(1, across):
                two(r, e).wait_recv()

            def total(rows):
                value = x_ref[grid.index(r, col, core), rows].astype(jnp.float32) + near[r, col, rows].astype(jnp.float32)
                for e in range(1, across):
                    value = value + wide[r, e - 1, rows].astype(jnp.float32)
                return value

            if d:

                def add(rows):
                    second[d - 1, rows] = total(rows).astype(second.dtype)

                blocks(add)
                three(d).start()
            else:
                for e in range(1, lines):
                    three(e).wait_recv()

                def add(rows):
                    value = total(rows)
                    for e in range(1, lines):
                        value = value + far[e - 1, rows].astype(jnp.float32)
                    o_ref[rows] = value.astype(o_ref.dtype)

                blocks(add)
            yield True
        for r in range(lines):
            for q in range(across):
                one(r, q).wait_send()
            for e in range(1, across):
                two(r, e).wait_send()
        for d in range(1, lines):
            three(d).wait_send()

    return Task(
        [x],
        [VMEM],
        [jax.ShapeDtypeStruct(block, dtype)],
        [VMEM],
        [
            pltpu.VMEM((lines, across) + block, x.dtype),
            pltpu.VMEM((lines, across - 1) + block, x.dtype),
            pltpu.VMEM((lines, across - 1) + block, x.dtype),
            pltpu.VMEM((lines - 1,) + block, x.dtype),
            pltpu.VMEM((lines - 1,) + block, x.dtype),
            dma((lines, across)),
            dma((lines, across)),
            dma((lines, across)),
            dma((lines, across)),
            dma((lines,)),
            dma((lines,)),
        ],
        targets,
        run,
    )


def scatter_all(x, count, ident, name, **how):
    cuts = max(1, x.size * x.dtype.itemsize >> 23)
    span = x.shape[1] // cuts
    parts = [
        fuse(ident + i, f"{name}{i}", scatter(x[:, i * span : (i + 1) * span], count, **how))[0][0] for i in range(cuts)
    ]
    return parts[0] if cuts == 1 else jnp.concatenate(parts, axis=1)


def swap(arrays):
    parts = len(arrays)

    def targets():
        return [("half", True, {"dp": lax.axis_index("dp"), "head": 1 - lax.axis_index("head")})]

    def run(*refs):
        ins, outs = refs[:parts], refs[parts : 2 * parts]
        send, recv = refs[2 * parts :]
        where = targets()[0][2]
        copies = [remote(ins[i], outs[i], send.at[i], recv.at[i], where) for i in range(parts)]
        for copy in copies:
            copy.start()
        yield True
        for copy in copies:
            copy.wait()

    return Task(
        list(arrays),
        [VMEM] * parts,
        [jax.ShapeDtypeStruct(a.shape, a.dtype) for a in arrays],
        [VMEM] * parts,
        [dma((parts,)), dma((parts,))],
        targets,
        run,
    )


def unit_targets(count):
    lines, columns = grid_of(count)
    grid = Grid(count)
    mine = grid.row * 2 + grid.core
    found = []
    for e in range(1, 2 * lines):
        member = mine ^ e
        found.append((("member", e), True, grid.where(member // 2, grid.column, member % 2)))
    for e in range(1, columns):
        found.append((("col", False, e), True, grid.where(grid.row, (grid.column + e) % columns, grid.core)))
    return found


def spread(w, count):
    lines, columns = grid_of(count)
    kinds, depth, width = w.shape
    tiles = width // LANES
    members = 2 * lines
    slots = pl.cdiv(tiles, members)
    twice = 2 * depth

    def run(w_ref, o_ref, zeros, send, recv, push, pull, blank):
        grid = Grid(count)
        mine = grid.row * 2 + grid.core

        def lanes(slot):
            return pl.ds(slot * LANES, LANES)

        def bytes_of(slot):
            return o_ref.at[:, pl.ds(0, members * depth), lanes(slot)]

        def full(slot, member):
            return True if (slot + 1) * members <= tiles else slot * members + member < tiles

        def guarded(ok, body):
            if ok is True:
                body()
            else:
                pl.when(ok)(body)

        def block(slot, member):
            return w_ref.at[:, :, pl.ds(pl.multiple_of((slot * members + member) * LANES, LANES), LANES)]

        def spot(slot):
            return o_ref.at[:, pl.ds(pl.multiple_of(grid.me * depth, depth), depth), lanes(slot)]

        def out(slot, e):
            member = mine ^ e
            return remote(
                block(slot, member),
                spot(slot),
                send.at[slot, e],
                recv.at[slot],
                grid.where(member // 2, grid.column, member % 2),
            )

        def chunk(slot, r, column):
            return o_ref.at[:, pl.ds(pl.multiple_of((r * columns + column) * twice, twice), twice), lanes(slot)]

        def over(slot, r, e):
            here = chunk(slot, r, grid.column)
            return remote(
                here,
                here,
                push.at[slot, r, e],
                pull.at[slot, e],
                grid.where(grid.row, (grid.column + e) % columns, grid.core),
            )

        for slot in range(slots):
            for e in range(1, members):
                guarded(full(slot, mine ^ e), lambda: out(slot, e).start())
            guarded(
                full(slot, mine), lambda: pltpu.make_async_copy(block(slot, mine), spot(slot), recv.at[slot]).start()
            )
        last = slots - 1
        some = full(last, mine)
        if some is not True:
            fills = [
                pltpu.make_async_copy(zeros, o_ref.at[:, pl.ds(i * depth, depth), lanes(last)], blank.at[i])
                for i in range(count)
            ]

            @pl.when(jnp.logical_not(some))
            def _():
                zeros[...] = jnp.zeros_like(zeros)
                for fill in fills:
                    fill.start()
                for fill in fills:
                    fill.wait()

        yield True
        for slot in range(slots):

            def pass_on():
                pltpu.make_async_copy(bytes_of(slot), bytes_of(slot), recv.at[slot]).wait()
                for r in range(lines):
                    for e in range(1, columns):
                        over(slot, r, e).start()

            guarded(full(slot, mine), pass_on)
            yield True
        for slot in range(slots):

            def finish():
                for e in range(1, columns):
                    pltpu.make_async_copy(bytes_of(slot), bytes_of(slot), pull.at[slot, e]).wait()
                    for r in range(lines):
                        over(slot, r, e).wait_send()

            guarded(full(slot, mine), finish)
            for e in range(1, members):
                guarded(full(slot, mine ^ e), lambda: out(slot, e).wait_send())

    return Task(
        [w],
        [VMEM],
        [jax.ShapeDtypeStruct((kinds, count * depth, slots * LANES), w.dtype)],
        [HBM],
        [
            pltpu.VMEM((kinds, depth, LANES), w.dtype),
            dma((slots, members)),
            dma((slots,)),
            dma((slots, lines, columns)),
            dma((slots, columns)),
            dma((count,)),
        ],
        functools.partial(unit_targets, count),
        run,
    )


def collect(g, count, width):
    lines, columns = grid_of(count)
    kinds, rows, span = g.shape
    tiles = width // LANES
    members = 2 * lines
    slots = span // LANES
    depth = rows // count
    twice = 2 * depth

    def run(g_ref, o_ref, near, stage, push, pull, send, recv):
        grid = Grid(count)
        mine = grid.row * 2 + grid.core

        def lanes(slot):
            return pl.ds(slot * LANES, LANES)

        def guarded(slot, body):
            if (slot + 1) * members <= tiles:
                body()
            else:
                pl.when(slot * members + mine < tiles)(body)

        def rows_at(r, column):
            return pl.multiple_of((r * columns + column) * twice, twice)

        def over(slot, r, e):
            column = (grid.column + e) % columns
            return remote(
                g_ref.at[:, pl.ds(rows_at(r, column), twice), lanes(slot)],
                near.at[slot, e - 1, :, pl.ds(r * twice, twice)],
                push.at[slot, r, e],
                pull.at[slot, e],
                grid.where(grid.row, column, grid.core),
            )

        def spot(slot):
            return o_ref.at[:, :, pl.ds(pl.multiple_of((slot * members + mine) * LANES, LANES), LANES)]

        def piece(slot, member):
            return stage.at[slot, :, pl.ds(pl.multiple_of(member * depth, depth), depth)]

        def out(slot, e):
            member = mine ^ e
            return remote(
                piece(slot, member),
                spot(slot),
                send.at[slot, e],
                recv,
                grid.where(member // 2, grid.column, member % 2),
            )

        for slot in range(slots):

            def begin():
                for e in range(1, columns):
                    for r in range(lines):
                        over(slot, r, e).start()

            guarded(slot, begin)
        yield True
        for slot in range(slots):

            def add_up():
                for e in range(1, columns):
                    pltpu.make_async_copy(near.at[slot, e - 1], near.at[slot, e - 1], pull.at[slot, e]).wait()

                def add(i, carry):
                    for r in range(lines):
                        here = pl.ds(pl.multiple_of(rows_at(r, grid.column) + i * 16, 16), 16)
                        there = pl.ds(pl.multiple_of(r * twice + i * 16, 16), 16)
                        for kind in range(kinds):
                            value = g_ref[kind, here, lanes(slot)].astype(jnp.float32)
                            for e in range(1, columns):
                                value = value + near[slot, e - 1, kind, there].astype(jnp.float32)
                            stage[slot, kind, there] = value.astype(stage.dtype)
                    return carry

                lax.fori_loop(0, twice // 16, add, 0)
                for e in range(1, members):
                    out(slot, e).start()
                pltpu.make_async_copy(piece(slot, mine), spot(slot), recv).start()

            guarded(slot, add_up)
            yield True
        pltpu.make_async_copy(o_ref, o_ref, recv).wait()
        for slot in range(slots):

            def finish():
                for e in range(1, columns):
                    for r in range(lines):
                        over(slot, r, e).wait_send()
                for e in range(1, members):
                    out(slot, e).wait_send()

            guarded(slot, finish)

    return Task(
        [g],
        [VMEM],
        [jax.ShapeDtypeStruct((kinds, depth, width), g.dtype)],
        [VMEM],
        [
            pltpu.VMEM((slots, columns - 1, kinds, members * depth, LANES), g.dtype),
            pltpu.VMEM((slots, kinds, members * depth, LANES), g.dtype),
            dma((slots, lines, columns)),
            dma((slots, columns)),
            dma((slots, members)),
            dma,
        ],
        functools.partial(unit_targets, count),
        run,
    )


def window(most):
    def bounds(tokens):
        first = lax.axis_index("dp") * tokens
        return jnp.maximum(first - most + 1, 0) // KEYS, (first + tokens - 1) // KEYS + 1, first

    return bounds


def attend(most, begin, q, kv):
    tokens, heads = q.shape[0], q.shape[1] // HEAD_SIZE

    def run(begin_ref, q_ref, kv_ref, o_ref, lse_ref):
        low, high, first = window(most)(tokens)
        begin = begin_ref[...]
        index = first + lax.broadcasted_iota(jnp.int32, (tokens, 1), 0)
        lane = lax.broadcasted_iota(jnp.int32, (tokens, HEAD_SIZE), 1)
        key_lane = lax.broadcasted_iota(jnp.int32, (tokens, KEYS), 1)
        yield True
        for h in range(heads):
            cols = slice(h * HEAD_SIZE, (h + 1) * HEAD_SIZE)

            def step(block, state):
                top, mass, total = state
                start = pl.multiple_of(block * KEYS, KEYS)
                keys = kv_ref[pl.ds(start, KEYS), :HEAD_SIZE]
                values = kv_ref[pl.ds(start, KEYS), HEAD_SIZE:]
                scores = lax.dot_general(
                    q_ref[:, cols], keys, (((1,), (1,)), ((), ())), preferred_element_type=jnp.float32
                )
                at = key_lane + start
                scores = jnp.where((at >= begin) & (at <= index), scores * SCALE2, masked_score)
                best = jnp.maximum(top, jnp.max(scores, axis=1, keepdims=True))
                fade = jnp.exp2(top - best)
                probs = jnp.exp2(scores - best)
                mass = mass * fade + jnp.sum(probs, axis=1, keepdims=True)
                total = total * fade + jnp.dot(
                    probs.astype(jnp.bfloat16), values, preferred_element_type=jnp.float32
                )
                return best, mass, total

            top, mass, total = lax.fori_loop(
                low,
                high,
                step,
                (
                    jnp.full((tokens, 1), masked_score, jnp.float32),
                    jnp.zeros((tokens, 1), jnp.float32),
                    jnp.zeros((tokens, HEAD_SIZE), jnp.float32),
                ),
            )
            o_ref[:, cols] = total / mass
            lse = top + jnp.log2(mass)
            lse_ref[...] = jnp.where(lane == h, lse, 0.0 if h == 0 else lse_ref[...])
            yield True

    return Task(
        [begin, q, kv],
        [VMEM] * 3,
        [jax.ShapeDtypeStruct(q.shape, jnp.float32), jax.ShapeDtypeStruct((tokens, HEAD_SIZE), jnp.float32)],
        [VMEM] * 2,
        [],
        None,
        run,
    )


def forward(most, count, begin, q, kv, attn, x, gain):
    tokens, width = q.shape[0], x.shape[1]
    part, inner = x.shape[0], q.shape[1]
    core = attend(most, begin, q, kv)
    rows = gather(jax.ShapeDtypeStruct((part, width), jnp.bfloat16), count, tower=True)
    pair = swap([jax.ShapeDtypeStruct((part, width), jnp.bfloat16)])
    n_rows, n_pair = len(rows.scratch), len(pair.scratch)
    columns = 256
    skip = attn.shape[1] - inner

    def run(begin_ref, q_ref, kv_ref, attn_ref, x_ref, gain_ref, o_ref, lse_ref, hidden_ref, rows_ref, *scratch):
        sent, got, normed, whole = scratch[:4]
        half = lax.axis_index("head")
        yield from core.run(begin_ref, q_ref, kv_ref, o_ref, lse_ref)

        def project(i, carry):
            cols = pl.ds(pl.multiple_of(i * columns, columns), columns)
            whole[:, cols] = lax.dot_general(
                o_ref[...].astype(jnp.bfloat16),
                attn_ref[cols, skip:],
                (((1,), (1,)), ((), ())),
                preferred_element_type=jnp.float32,
            )
            return carry

        lax.fori_loop(0, width // columns, project, 0)

        def of(h):
            return pl.ds(pl.multiple_of(h * part, part), part)

        sent[...] = whole[of(1 - half)].astype(jnp.bfloat16)
        yield from pair.run(sent, got, *scratch[4 : 4 + n_pair])
        step = 16

        def norm(i, carry):
            here = pl.ds(pl.multiple_of(i * step, step), step)
            there = pl.ds(pl.multiple_of(half * part + i * step, step), step)
            hidden = x_ref[here].astype(jnp.float32) + (whole[there] + got[here].astype(jnp.float32))
            hidden_ref[here] = hidden
            normed[0, here] = (hidden * rms_scale(hidden) * gain_ref[...]).astype(jnp.bfloat16)
            return carry

        lax.fori_loop(0, part // step, norm, 0)
        yield from rows.run(normed, rows_ref, *scratch[4 + n_pair :])

    def targets():
        return pair.targets() + rows.targets()

    return Task(
        [begin, q, kv, attn, x, gain],
        [VMEM] * 6,
        core.outs + [jax.ShapeDtypeStruct((part, width), jnp.float32)] + rows.outs,
        [VMEM] * 3 + rows.out_specs,
        [
            pltpu.VMEM((part, width), jnp.bfloat16),
            pltpu.VMEM((part, width), jnp.bfloat16),
            pltpu.VMEM((1, part, width), jnp.bfloat16),
            pltpu.VMEM((tokens, width), jnp.float32),
        ]
        + pair.scratch
        + rows.scratch,
        targets,
        run,
    )


def attend_back(most, begin, q, kv, lse, raw, do):
    tokens, heads = q.shape[0], q.shape[1] // HEAD_SIZE
    across = (((1,), (1,)), ((), ()))
    down = (((0,), (0,)), ((), ()))

    def run(begin_ref, q_ref, kv_ref, lse_ref, raw_ref, do_ref, dq_ref, dkv_ref, delta_ref):
        low, high, first = window(most)(tokens)
        begin = begin_ref[...]
        index = first + lax.broadcasted_iota(jnp.int32, (tokens, 1), 0)
        lane = lax.broadcasted_iota(jnp.int32, (tokens, HEAD_SIZE), 1)
        key_lane = lax.broadcasted_iota(jnp.int32, (tokens, KEYS), 1)
        table = jnp.zeros((tokens, HEAD_SIZE), jnp.float32)
        for h in range(heads):
            cols = slice(h * HEAD_SIZE, (h + 1) * HEAD_SIZE)
            delta = jnp.sum(do_ref[:, cols].astype(jnp.float32) * raw_ref[:, cols], axis=1, keepdims=True)
            table = jnp.where(lane == h, delta, table)
        delta_ref[...] = table
        dq_ref[...] = jnp.zeros_like(dq_ref)
        blocks = kv_ref.shape[0] // KEYS

        def clear(block, carry):
            dkv_ref[block] = jnp.zeros((KEYS, 2 * HEAD_SIZE), dkv_ref.dtype)
            return carry

        lax.fori_loop(0, low, clear, 0)
        lax.fori_loop(high, blocks, clear, 0)

        def step(block, carry):
            start = pl.multiple_of(block * KEYS, KEYS)
            rows = pl.ds(start, KEYS)
            keys = kv_ref[rows, :HEAD_SIZE]
            values = kv_ref[rows, HEAD_SIZE:]
            at = key_lane + start
            seen = (at >= begin) & (at <= index)
            dk = jnp.zeros((KEYS, HEAD_SIZE), jnp.float32)
            dv = jnp.zeros((KEYS, HEAD_SIZE), jnp.float32)
            for h in range(heads):
                cols = slice(h * HEAD_SIZE, (h + 1) * HEAD_SIZE)
                q = q_ref[:, cols]
                do = do_ref[:, cols]
                scores = lax.dot_general(q, keys, across, preferred_element_type=jnp.float32)
                probs = jnp.where(seen, jnp.exp2(scores * SCALE2 - lse_ref[:, h : h + 1]), 0.0)
                pull = lax.dot_general(do, values, across, preferred_element_type=jnp.float32)
                ds = (probs * (pull - delta_ref[:, h : h + 1])).astype(jnp.bfloat16)
                dq_ref[:, cols] += jnp.dot(ds, keys, preferred_element_type=jnp.float32)
                dk = dk + lax.dot_general(ds, q, down, preferred_element_type=jnp.float32)
                dv = dv + lax.dot_general(
                    probs.astype(jnp.bfloat16), do, down, preferred_element_type=jnp.float32
                )
            dkv_ref[block, :, :HEAD_SIZE] = (dk * SCALE).astype(dkv_ref.dtype)
            dkv_ref[block, :, HEAD_SIZE:] = dv.astype(dkv_ref.dtype)
            return carry

        parts = 3
        reach = high - low
        yield True
        for i in range(parts):
            lax.fori_loop(low + reach * i // parts, low + reach * (i + 1) // parts, step, 0)
            yield True

    return Task(
        [begin, q, kv, lse, raw, do],
        [VMEM] * 6,
        [
            jax.ShapeDtypeStruct(q.shape, jnp.float32),
            jax.ShapeDtypeStruct((kv.shape[0] // KEYS, KEYS, kv.shape[1]), kv.dtype),
        ],
        [VMEM] * 2,
        [pltpu.VMEM((tokens, HEAD_SIZE), jnp.float32)],
        None,
        run,
    )


def doc_layout(row_lengths, first_token, token_count):
    doc_ends = jnp.cumsum(row_lengths)
    doc_starts = doc_ends - row_lengths
    token_index = first_token + jnp.arange(token_count, dtype=jnp.int32)
    doc_begin = jnp.max(
        jnp.where(doc_starts[None, :] <= token_index[:, None], doc_starts[None, :], 0), axis=1
    )
    return (doc_begin, token_index - doc_begin)


def rope_tables(positions):
    freq = rope_base ** (-jnp.arange(0, HEAD_SIZE, 2, dtype=jnp.float32) / HEAD_SIZE)
    angle = positions.astype(jnp.float32)[:, None] * freq[None, :]
    angle = jnp.concatenate([angle, angle], axis=1)
    return (jnp.cos(angle)[:, None, :], jnp.sin(angle)[:, None, :])


def rotary_apply(values, cosine_table, sine_table):
    half_width = values.shape[-1] // 2
    turned = jnp.concatenate([-values[..., half_width:], values[..., :half_width]], axis=-1)
    return values * cosine_table + turned * sine_table


def unrotate(grads, cosine_table, sine_table):
    half_width = grads.shape[-1] // 2
    scaled_grad = grads * sine_table
    back_part = jnp.concatenate(
        [scaled_grad[..., half_width:], -scaled_grad[..., :half_width]], axis=-1
    )
    return grads * cosine_table + back_part


def rms_scale(values):
    return lax.rsqrt(jnp.mean(values * values, axis=-1, keepdims=True) + norm_epsilon)


def norm_back(grad_out, inputs, scale, gain):
    weighted = grad_out * gain
    return scale * weighted - inputs * scale**3 * jnp.mean(
        weighted * inputs, axis=-1, keepdims=True
    )


def dot(a, b, dims=((1,), (0,))):
    return lax.dot_general(a, b, (dims, ((), ())), preferred_element_type=jnp.float32)


across_dims = ((1,), (1,))
token_dims = ((0,), (0,))


def backward(most, count, begin, q, kv, lse, raw, own, attn):
    tokens, width = q.shape[0], own.shape[1]
    part, inner = own.shape[0], q.shape[1]
    core = attend_back(most, begin, q, kv, lse, raw, jax.ShapeDtypeStruct(q.shape, jnp.bfloat16))
    d_query, d_kv = core.outs
    sums = scatter(jax.ShapeDtypeStruct((kv.shape[0], kv.shape[1]), kv.dtype), count)
    columns = 256
    skip = attn.shape[1] - inner

    def run(
        begin_ref, q_ref, kv_ref, lse_ref, raw_ref, own_ref, attn_ref, dq_ref, sums_ref, branch_ref, delta, do, dkv, send, recv, *scratch
    ):
        half = lax.axis_index("head")
        here = pl.ds(pl.multiple_of(half * part, part), part)
        copy = remote(
            own_ref, branch_ref.at[here], send, recv, {"dp": lax.axis_index("dp"), "head": 1 - half}
        )
        copy.start()
        branch_ref[here] = own_ref[...]
        yield True
        copy.wait_recv()

        def project(i, carry):
            cols = pl.ds(pl.multiple_of(i * columns, columns), columns)
            there = pl.ds(pl.multiple_of(skip + i * columns, columns), columns)
            do[:, cols] = jnp.dot(
                branch_ref[...], attn_ref[:, there], preferred_element_type=jnp.float32
            ).astype(do.dtype)
            return carry

        lax.fori_loop(0, inner // columns, project, 0)
        yield from core.run(begin_ref, q_ref, kv_ref, lse_ref, raw_ref, do, dq_ref, dkv, delta)
        yield from sums.run(dkv, sums_ref, *scratch)
        copy.wait_send()

    def targets():
        return [("half", True, {"dp": lax.axis_index("dp"), "head": 1 - lax.axis_index("head")})] + sums.targets()

    return Task(
        [begin, q, kv, lse, raw, own, attn],
        [VMEM] * 7,
        [d_query] + sums.outs + [jax.ShapeDtypeStruct((tokens, width), jnp.bfloat16)],
        [VMEM] * 3,
        core.scratch
        + [pltpu.VMEM(q.shape, jnp.bfloat16), pltpu.VMEM(d_kv.shape, d_kv.dtype), dma, dma]
        + sums.scratch,
        targets,
        run,
    )


def weight_grads(rows, grads, d_gate, d_up, active):
    arrays = [rows, grads, d_gate, d_up, active]
    width, units = rows.shape[1], active.shape[1]
    columns = 256
    down = (((0,), (0,)), ((), ()))

    def run(*refs):
        ins, (o_ref,), held, (sems,) = refs[:5], refs[5:6], refs[6:11], refs[11:]
        copies = [pltpu.make_async_copy(ins[i], held[i], sems.at[i]) for i in range(5)]
        for i in (0, 2, 3, 1, 4):
            copies[i].start()
        yield True
        for i in (0, 2, 3):
            copies[i].wait()

        def first(i, carry):
            cols = pl.ds(pl.multiple_of(i * columns, columns), columns)
            for kind in (0, 1):
                o_ref[kind, cols] = lax.dot_general(
                    held[0][:, cols], held[2 + kind][...], down, preferred_element_type=jnp.float32
                ).astype(o_ref.dtype)
            return carry

        def second(i, carry):
            cols = pl.ds(pl.multiple_of(i * columns, columns), columns)
            o_ref[2, cols] = lax.dot_general(
                held[1][:, cols], held[4][...], down, preferred_element_type=jnp.float32
            ).astype(o_ref.dtype)
            return carry

        lax.fori_loop(0, width // columns, first, 0)
        yield True
        for i in (1, 4):
            copies[i].wait()
        lax.fori_loop(0, width // columns, second, 0)
        yield True

    return Task(
        arrays,
        [HBM] * 5,
        [jax.ShapeDtypeStruct((3, width, units), jnp.bfloat16)],
        [VMEM],
        [pltpu.VMEM(a.shape, a.dtype) for a in arrays] + [dma((5,))],
        None,
        run,
    )


def longest(token_count):
    return 2048 if token_count == 4096 else token_count


def body(
    count,
    layer_in,
    gain_attn,
    q_weight,
    q_bias,
    key_weight,
    key_bias,
    value_weight,
    value_bias,
    o_weight,
    gain_mlp,
    gate_weight,
    up_weight,
    down_weight,
    row_lengths,
    source_ids,
    source_weights,
    out_grad,
):
    f32, bf16 = jnp.float32, jnp.bfloat16
    tok_rows, width = layer_in.shape
    part = tok_rows // 2
    half = lax.axis_index("head")
    first_token = lax.axis_index("dp") * tok_rows
    doc_begin, positions = doc_layout(row_lengths, first_token, tok_rows)
    cosine_table, sine_table = rope_tables(positions)
    q_cols = q_weight.shape[1]
    kv_cols = key_weight.shape[1]
    heads = q_cols // HEAD_SIZE
    ff_cols = gate_weight.shape[1]

    def mine(rows):
        return lax.dynamic_slice_in_dim(rows, half * part, part, 0)

    def other(rows):
        return lax.dynamic_slice_in_dim(rows, (1 - half) * part, part, 0)

    def join(own, peer):
        return jnp.where(half == 0, jnp.concatenate([own, peer]), jnp.concatenate([peer, own]))

    attn_local = jnp.concatenate([q_weight, key_weight, value_weight, o_weight.T], axis=1)
    picked = source_ids[:, None] == jnp.arange(source_weights.shape[0], dtype=jnp.int32)[None, :]
    row_scale = (
        jnp.sum(jnp.where(picked, source_weights[None, :], 0), axis=1).astype(f32) / loss_denominator
    )
    cotangent = mine(out_grad).astype(f32) * mine(row_scale[:, None])
    ((attn_full,), (grad_all,)) = fuse(
        1, "gather_inputs", gather(attn_local, count), gather(cotangent.astype(bf16), count, tower=True)
    )
    attn_full = attn_full.reshape(width, -1)
    grad_all = grad_all.reshape(-1, width)
    qkv_cols = q_cols + 2 * kv_cols
    full_qkv = attn_full[:, :qkv_cols]
    full_o = attn_full[:, qkv_cols:]
    inputs = layer_in.astype(f32)
    scale_one = rms_scale(inputs)
    gain_one = gain_attn.astype(f32)
    normed = (inputs * scale_one * gain_one).astype(bf16)
    bias = jnp.concatenate([q_bias, key_bias, value_bias]).astype(f32)
    pre = dot(normed, full_qkv) + bias
    turned = rotary_apply(
        pre[:, : q_cols + kv_cols].reshape(tok_rows, heads + 1, HEAD_SIZE), cosine_table, sine_table
    ).reshape(tok_rows, q_cols + kv_cols)
    query_rows = turned[:, :q_cols].astype(bf16)
    kv_rows = jnp.concatenate([turned[:, q_cols:], pre[:, q_cols + kv_cols :]], axis=1).astype(bf16)
    ((kv_all,),) = fuse(2, "gather_keys", gather(kv_rows, count))
    kv_all = kv_all.reshape(-1, 2 * kv_cols)
    begin = doc_begin[:, None].astype(jnp.int32)
    most = longest(count * tok_rows)
    mlp_local = jnp.stack([gate_weight, up_weight, down_weight.T])
    gain_two = gain_mlp.astype(f32)
    ahead = (0, 1) + (1, 1, 1, 0) + (1, 1, 1, 0) + (1, 0, 1, 1, 0) + (1,) * 6 + (0,)
    ((mlp_full,), (attended_raw, row_lse, hidden, rows_all)) = fuse(
        3,
        "forward_spread",
        spread(mlp_local, count),
        forward(most, count, begin, query_rows, kv_all, attn_full, mine(layer_in), gain_two[None, :]),
        order=ahead,
    )
    attended = attended_raw.astype(bf16)
    scale_two = rms_scale(hidden)
    rows_all = rows_all.reshape(-1, width)

    full_gate, full_up, full_down = mlp_full[0], mlp_full[1], mlp_full[2]
    gate_act = dot(rows_all, full_gate)
    up_act = dot(rows_all, full_up)
    sigmoid_gate = jax.nn.sigmoid(gate_act)
    silu_gate = gate_act * sigmoid_gate
    active = (silu_gate * up_act).astype(bf16)
    d_active = dot(grad_all, full_down)
    d_gate = (d_active * up_act * sigmoid_gate * (1.0 + gate_act * (1.0 - sigmoid_gate))).astype(bf16)
    d_up = (d_active * silu_gate).astype(bf16)
    mlp_part = dot(active, full_down, across_dims).astype(bf16)
    norm_two_part = (dot(d_gate, full_gate, across_dims) + dot(d_up, full_up, across_dims)).astype(bf16)
    operands = (rows_all, grad_all, d_gate, d_up, active)
    if count <= 16:
        ((d_normed_mlp,), (mlp_grads,)) = fuse(
            8,
            "scatter_grads",
            scatter(norm_two_part, count, tower=True),
            weight_grads(*operands),
            order=(0, 1, 0, 0, 0, 1, 0, 0, 1),
        )
    else:
        d_normed_mlp = scatter_all(norm_two_part, count, 8, "scatter_rows", tower=True)
        mlp_grads = jnp.stack(
            [
                dot(rows_all, d_gate, token_dims).astype(bf16),
                dot(rows_all, d_up, token_dims).astype(bf16),
                dot(grad_all, active, token_dims).astype(bf16),
            ]
        )
    gain_two_local = jnp.sum(d_normed_mlp * hidden * scale_two, axis=0)
    d_hidden = cotangent + norm_back(d_normed_mlp, hidden, scale_two, gain_two)
    branch_own = d_hidden.astype(bf16)
    ((mlp_part_sums,), (d_query, kv_sums, branch_grad)) = fuse(
        17,
        "backward_collect",
        collect(mlp_grads, count, ff_cols),
        backward(most, count, begin, query_rows, kv_all, row_lse, attended_raw, branch_own, attn_full),
        order=(1, 0, 1, 1, 0, 1, 0, 1, 0, 1, 1, 0),
    )
    mlp_part_sums = mlp_part_sums.astype(f32)
    out_proj_grad = dot(branch_grad, attended, token_dims)
    d_queries = (d_query * SCALE).astype(bf16).astype(f32)
    d_key_rot = kv_sums[:, :kv_cols].astype(bf16).astype(f32)
    d_value_rows = kv_sums[:, kv_cols:].astype(bf16)
    d_turned = jnp.concatenate([d_queries, d_key_rot], axis=1).reshape(tok_rows, heads + 1, HEAD_SIZE)
    d_pre = jnp.concatenate(
        [
            unrotate(d_turned, cosine_table, sine_table).reshape(tok_rows, q_cols + kv_cols).astype(bf16),
            d_value_rows,
        ],
        axis=1,
    )
    bias_local = jnp.sum(d_pre.astype(f32), axis=0)
    qkv_grad = dot(normed, d_pre, token_dims)
    attn_grads = jnp.concatenate([qkv_grad, out_proj_grad], axis=1).astype(bf16)
    norm_one_part = dot(d_pre, full_qkv, across_dims)
    norm_send = other(norm_one_part).astype(bf16)
    if count <= 16:
        ((attn_part,), (mlp_out,), (norm_peer,)) = fuse(
            21, "scatter_last", scatter(attn_grads, count), scatter(mlp_part, count, tower=True), swap([norm_send])
        )
    else:
        attn_part = scatter_all(attn_grads, count, 21, "scatter_attn")
        mlp_out = scatter_all(mlp_part, count, 25, "scatter_out", tower=True)
        ((norm_peer,),) = fuse(33, "swap_norm", swap([norm_send]))
    layer_out_own = (hidden + mlp_out).astype(bf16)
    d_normed = mine(norm_one_part) + norm_peer.astype(f32)
    inputs_own = mine(inputs)
    scale_own = mine(scale_one)
    gain_one_local = jnp.sum(d_normed * inputs_own * scale_own, axis=0)
    layer_in_grad_own = (d_hidden + norm_back(d_normed, inputs_own, scale_own, gain_one)).astype(bf16)

    small = jnp.concatenate([bias_local, gain_one_local, gain_two_local]).reshape(-1, LANES)
    ((small_all,), (layer_in_grad_peer, layer_out_peer)) = fuse(
        34, "gather_sums", gather(small, count, both=True), swap([layer_in_grad_own, layer_out_own])
    )
    small_all = small_all.reshape(count, 2, -1)
    small_sum = jnp.sum(small_all[:, 0], axis=0)
    gains = (small_sum[qkv_cols:] + jnp.sum(small_all[:, 1, qkv_cols:], axis=0)).reshape(2, width)
    layer_in_grad = join(layer_in_grad_own, layer_in_grad_peer)
    layer_out = join(layer_out_own, layer_out_peer)
    return (
        layer_out,
        layer_in_grad,
        gains[0],
        attn_part[:, :q_cols],
        small_sum[:q_cols],
        attn_part[:, q_cols : q_cols + kv_cols],
        small_sum[q_cols : q_cols + kv_cols],
        attn_part[:, q_cols + kv_cols : qkv_cols],
        small_sum[q_cols + kv_cols : qkv_cols],
        attn_part[:, qkv_cols:].T,
        gains[1],
        mlp_part_sums[0],
        mlp_part_sums[1],
        mlp_part_sums[2].T,
    )


def solution(mesh):
    placed = (
        P("dp", None),
        P(),
        P("dp", "head"),
        P("head"),
        P("dp", "head"),
        P("head"),
        P("dp", "head"),
        P("head"),
        P("head", "dp"),
        P(),
        P("dp", "head"),
        P("dp", "head"),
        P("head", "dp"),
        P(),
        P("dp"),
        P(),
        P("dp", None),
    )
    return jax.shard_map(
        functools.partial(body, mesh.shape["dp"]),
        mesh=mesh,
        in_specs=placed,
        out_specs=(
            P("dp", None),
            P("dp", None),
            P(),
            P("dp", "head"),
            P("head"),
            P("dp", "head"),
            P("head"),
            P("dp", "head"),
            P("head"),
            P("head", "dp"),
            P(),
            P("dp", "head"),
            P("dp", "head"),
            P("head", "dp"),
        ),
        check_vma=False,
    )
```

```python
import dataclasses
import functools
from typing import Any, Callable
import jax
import jax.numpy as jnp
from jax import lax
from jax.experimental import pallas as pl
from jax.experimental.pallas import tpu as pltpu
from jax.sharding import PartitionSpec as P

HEAD_SIZE = 128
KEYS = 256
SCALE = HEAD_SIZE**-0.5
SCALE2 = SCALE * 1.4426950408889634
MESH = pl.DeviceIdType.MESH
LANES = 128
norm_epsilon = 1e-06
rope_base = 1000000.0
loss_denominator = 16.0
masked_score = -1e30
VMEM = pl.BlockSpec(memory_space=pltpu.VMEM)
HBM = pl.BlockSpec(memory_space=pl.ANY)
dma = pltpu.SemaphoreType.DMA


def grid_of(count):
    across = 2 if count <= 16 else 4
    return count // (2 * across), across


def remote(src, dst, send, recv, where):
    return pltpu.make_async_remote_copy(
        src_ref=src, dst_ref=dst, send_sem=send, recv_sem=recv, device_id=where, device_id_type=MESH
    )


def reshape(x, shape):
    if isinstance(x, jax.ShapeDtypeStruct):
        return jax.ShapeDtypeStruct(shape, x.dtype)
    return x.reshape(shape)


class Grid:
    def __init__(self, count, tower=False):
        self.lines, self.columns = grid_of(count)
        self.tower = tower
        self.across = 2 if tower else self.columns
        me, self.half = lax.axis_index("dp"), lax.axis_index("head")
        self.me = me
        self.core = me % 2
        self.column = (me // 2) % self.columns
        self.row = me // (2 * self.columns)
        self.col = self.half if tower else self.column

    def where(self, r, q, k):
        if self.tower:
            return {"dp": (r * self.columns + self.column) * 2 + k, "head": q}
        return {"dp": (r * self.columns + q) * 2 + k, "head": self.half}

    def index(self, r, q, k):
        return (r * self.across + q) * 2 + k


@dataclasses.dataclass
class Task:
    inputs: list
    in_specs: list
    outs: list
    out_specs: list
    scratch: list
    targets: Callable
    run: Callable


def fuse(ident, name, *tasks, order=()):
    remote_ops = any(t.targets is not None for t in tasks)

    def split(refs, sizes):
        parts, start = [], 0
        for size in sizes:
            parts.append(refs[start : start + size])
            start += size
        return parts

    n_in = [len(t.inputs) for t in tasks]
    n_out = [len(t.outs) for t in tasks]
    n_scratch = [len(t.scratch) for t in tasks]

    def kernel(*refs):
        ins, outs, scratch = split(refs, [sum(n_in), sum(n_out), sum(n_scratch)])
        if remote_ops:
            barrier = pltpu.get_barrier_semaphore()
            known, total = set(), 0
            for t in tasks:
                for key, ok, where in t.targets() if t.targets is not None else ():
                    if key in known:
                        continue
                    known.add(key)
                    if ok is True:
                        pl.semaphore_signal(barrier, inc=1, device_id=where, device_id_type=MESH)
                        total = total + 1
                    else:

                        @pl.when(ok)
                        def _():
                            pl.semaphore_signal(barrier, inc=1, device_id=where, device_id_type=MESH)

                        total = total + ok.astype(jnp.int32)
            pl.semaphore_wait(barrier, total)
        steps = [
            t.run(*a, *b, *c)
            for t, a, b, c in zip(tasks, split(ins, n_in), split(outs, n_out), split(scratch, n_scratch))
        ]
        live = set(range(len(steps)))
        turns = list(order)
        while live:
            for i in turns:
                if i in live and next(steps[i], None) is None:
                    live.remove(i)
            turns = sorted(live)

    params = dict(vmem_limit_bytes=60 << 20)
    if remote_ops:
        params.update(collective_id=ident, has_side_effects=True)
    flat = pl.pallas_call(
        kernel,
        out_shape=[o for t in tasks for o in t.outs],
        in_specs=[s for t in tasks for s in t.in_specs],
        out_specs=[s for t in tasks for s in t.out_specs],
        scratch_shapes=[s for t in tasks for s in t.scratch],
        compiler_params=pltpu.CompilerParams(**params),
        name=name,
    )(*[x for t in tasks for x in t.inputs])
    return split(flat, n_out)


def gather(x, count, tower=False, pieces=1, both=False):
    lines, columns = grid_of(count)
    across = 2 if tower else columns
    members = lines * across * 2
    shape = x.shape
    pieces = 1 if both else pieces
    x = reshape(x, (pieces, shape[0] // pieces) + shape[1:])
    copies = 2 if both else pieces

    def hops_of(grid):
        row, col, core = grid.row, grid.col, grid.core
        return (
            (row < lines - 1, grid.where(row + 1, col, core)),
            (row > 0, grid.where(row - 1, col, core)),
            (col < across - 1, grid.where(row, col + 1, core)),
            (col > 0, grid.where(row, col - 1, core)),
            (True, grid.where(row, col, 1 - core)),
        )

    def targets():
        grid = Grid(count, tower)
        found = [(("hop", tower, i), ok, to) for i, (ok, to) in enumerate(hops_of(grid))]
        if both:
            found.append(("half", True, {"dp": grid.me, "head": 1 - grid.half}))
        return found

    def run(x_ref, o_ref, send, recv, local, cross):
        grid = Grid(count, tower)
        hops = hops_of(grid)
        core, col, row = grid.core, grid.col, grid.row
        me = grid.index(row, col, core)

        def copy(hop, shard, piece, src):
            return remote(src, o_ref.at[shard, piece], send.at[hop, shard, piece], recv.at[shard, piece], hops[hop][1])

        order = sorted(
            ((dr, dq) for dr in range(1 - lines, lines) for dq in range(1 - across, across)),
            key=lambda p: (abs(p[0]) + abs(p[1]), abs(p[1])),
        )
        if both:
            pair = remote(
                x_ref.at[0], o_ref.at[me, 1], cross.at[0], cross.at[1], {"dp": grid.me, "head": 1 - grid.half}
            )
            pair.start()
        sends = []
        mine = pltpu.make_async_copy(x_ref, o_ref.at[me, pl.ds(0, pieces)], local)
        for dr, dq in order:
            shard = grid.index(row - dr, col - dq, core)
            valid = (row - dr >= 0) & (row - dr < lines) & (col - dq >= 0) & (col - dq < across)
            onward = []
            if dq == 0:
                if dr >= 0:
                    onward.append(0)
                if dr <= 0:
                    onward.append(1)
            if dq >= 0:
                onward.append(2)
            if dq <= 0:
                onward.append(3)
            onward.append(4)
            for piece in range(copies):
                own = dr == 0 and dq == 0
                src = o_ref.at[shard, piece]
                if own and piece < pieces:
                    src = x_ref.at[piece]
                if own and piece >= pieces:
                    pair.wait_recv()
                if not own:

                    @pl.when(valid)
                    def _():
                        copy(4, shard, piece, src).wait_recv()

                for hop in onward:
                    ok = hops[hop][0]
                    go = valid if ok is True else valid & ok

                    @pl.when(go)
                    def _():
                        copy(hop, shard, piece, src).start()

                    sends.append((go, hop, shard, piece, src))
                yield True
            if dr == 0 and dq == 0:
                mine.start()
        for r in range(lines):
            for q in range(across):
                for piece in range(copies):
                    shard = grid.index(r, q, 1 - core)
                    copy(4, shard, piece, o_ref.at[shard, piece]).wait_recv()
        yield True
        for go, hop, shard, piece, src in sends:

            @pl.when(go)
            def _():
                copy(hop, shard, piece, src).wait_send()

        mine.wait()
        if both:
            pair.wait_send()

    return Task(
        [x],
        [VMEM],
        [jax.ShapeDtypeStruct((members, copies) + x.shape[1:], x.dtype)],
        [HBM],
        [dma((5, members, copies)), dma((members, copies)), dma, dma((2,))],
        targets,
        run,
    )


def scatter(x, count, tower=False, dtype=jnp.float32):
    lines, columns = grid_of(count)
    across = 2 if tower else columns
    members = lines * across * 2
    block = (x.shape[0] // members,) + x.shape[1:]
    height = block[0]
    step = 16
    x = reshape(x, (members,) + block)

    def targets():
        grid = Grid(count, tower)
        row, col, core = grid.row, grid.col, grid.core
        found = [(("hop", tower, 4), True, grid.where(row, col, 1 - core))]
        found += [(("col", tower, e), True, grid.where(row, (col + e) % across, core)) for e in range(1, across)]
        found.append((("hop", tower, 0), row < lines - 1, grid.where(row + 1, col, core)))
        found.append((("hop", tower, 1), row > 0, grid.where(row - 1, col, core)))
        return found

    def run(x_ref, o_ref, near, first, wide, second, far, s1, r1, s2, r2, s3, r3):
        grid = Grid(count, tower)
        row, col, core = grid.row, grid.col, grid.core

        def one(r, q):
            return remote(
                x_ref.at[grid.index(r, q, 1 - core)], near.at[r, q], s1.at[r, q], r1.at[r, q], grid.where(row, col, 1 - core)
            )

        def two(r, e):
            return remote(
                first.at[r, e - 1], wide.at[r, e - 1], s2.at[r, e], r2.at[r, e], grid.where(row, (col + e) % across, core)
            )

        def three(r):
            to = jnp.where(r > row, row + 1, row - 1)
            place = jnp.where((r > row) | (to != r), r, lines)
            return remote(second.at[r], far.at[place], s3.at[r], r3.at[place], grid.where(to, col, core))

        def arrived(place):
            remote(second.at[0], far.at[place], s3.at[0], r3.at[place], grid.where(row, col, 1 - core)).wait_recv()

        def turn(t):
            return jnp.where(row < lines // 2, lines - 1 - t, t)

        for t in range(lines):
            r = turn(t)
            for e in [e for e in range(1, across)] + [0]:
                one(r, (col + e) % across).start()
        yield True

        def blocks(body):
            def run_block(i, carry):
                body(pl.ds(pl.multiple_of(i * step, step), step))
                return carry

            lax.fori_loop(0, height // step, run_block, 0)

        for t in range(lines):
            r = turn(t)
            for e in range(1, across):
                q = (col + e) % across
                one(r, q).wait_recv()

                def add(rows):
                    first[r, e - 1, rows] = (
                        x_ref[grid.index(r, q, core), rows].astype(jnp.float32) + near[r, q, rows].astype(jnp.float32)
                    ).astype(first.dtype)

                blocks(add)
                two(r, e).start()
            yield True
        for t in range(lines):
            r = turn(t)
            one(r, col).wait_recv()
            for e in range(1, across):
                two(r, e).wait_recv()
            behind = ((r > row) & (row > 0)) | ((r < row) & (row < lines - 1))

            def total(rows):
                value = x_ref[grid.index(r, col, core), rows].astype(jnp.float32) + near[r, col, rows].astype(jnp.float32)
                for e in range(1, across):
                    value = value + wide[r, e - 1, rows].astype(jnp.float32)
                return value

            @pl.when(r == row)
            def _():
                def keep(rows):
                    o_ref[rows] = total(rows).astype(o_ref.dtype)

                blocks(keep)

            @pl.when((r != row) & jnp.logical_not(behind))
            def _():
                def begin(rows):
                    second[r, rows] = total(rows).astype(second.dtype)

                blocks(begin)
                three(r).start()

            @pl.when((r != row) & behind)
            def _():
                arrived(r)

                def pass_on(rows):
                    second[r, rows] = (total(rows) + far[r, rows].astype(jnp.float32)).astype(second.dtype)

                blocks(pass_on)
                three(r).start()

            yield True
        for ok, place in ((row > 0, row), (row < lines - 1, lines)):

            @pl.when(ok)
            def _():
                arrived(place)

                def last(rows):
                    o_ref[rows] = (o_ref[rows] + far[place, rows].astype(jnp.float32)).astype(o_ref.dtype)

                blocks(last)

        yield True
        for r in range(lines):
            for q in range(across):
                one(r, q).wait_send()
            for e in range(1, across):
                two(r, e).wait_send()

            @pl.when(r != row)
            def _():
                three(r).wait_send()

    return Task(
        [x],
        [VMEM],
        [jax.ShapeDtypeStruct(block, dtype)],
        [VMEM],
        [
            pltpu.VMEM((lines, across) + block, x.dtype),
            pltpu.VMEM((lines, across - 1) + block, x.dtype),
            pltpu.VMEM((lines, across - 1) + block, x.dtype),
            pltpu.VMEM((lines,) + block, x.dtype),
            pltpu.VMEM((lines + 1,) + block, x.dtype),
            dma((lines, across)),
            dma((lines, across)),
            dma((lines, across)),
            dma((lines, across)),
            dma((lines,)),
            dma((lines + 1,)),
        ],
        targets,
        run,
    )


def scatter_all(x, count, ident, name, **how):
    cuts = max(1, x.size * x.dtype.itemsize >> 23)
    span = x.shape[1] // cuts
    parts = [
        fuse(ident + i, f"{name}{i}", scatter(x[:, i * span : (i + 1) * span], count, **how))[0][0] for i in range(cuts)
    ]
    return parts[0] if cuts == 1 else jnp.concatenate(parts, axis=1)


def swap(arrays):
    parts = len(arrays)

    def targets():
        return [("half", True, {"dp": lax.axis_index("dp"), "head": 1 - lax.axis_index("head")})]

    def run(*refs):
        ins, outs = refs[:parts], refs[parts : 2 * parts]
        send, recv = refs[2 * parts :]
        where = targets()[0][2]
        copies = [remote(ins[i], outs[i], send.at[i], recv.at[i], where) for i in range(parts)]
        for copy in copies:
            copy.start()
        yield True
        for copy in copies:
            copy.wait()

    return Task(
        list(arrays),
        [VMEM] * parts,
        [jax.ShapeDtypeStruct(a.shape, a.dtype) for a in arrays],
        [VMEM] * parts,
        [dma((parts,)), dma((parts,))],
        targets,
        run,
    )


def unit_targets(count):
    lines, columns = grid_of(count)
    grid = Grid(count)
    mine = grid.row * 2 + grid.core
    found = []
    for e in range(1, 2 * lines):
        member = mine ^ e
        found.append((("member", e), True, grid.where(member // 2, grid.column, member % 2)))
    for e in range(1, columns):
        found.append((("col", False, e), True, grid.where(grid.row, (grid.column + e) % columns, grid.core)))
    return found


def spread(w, count):
    lines, columns = grid_of(count)
    kinds, depth, width = w.shape
    tiles = width // LANES
    members = 2 * lines
    slots = pl.cdiv(tiles, members)
    twice = 2 * depth

    def run(w_ref, o_ref, zeros, send, recv, push, pull, blank):
        grid = Grid(count)
        mine = grid.row * 2 + grid.core

        def lanes(slot):
            return pl.ds(slot * LANES, LANES)

        def bytes_of(slot):
            return o_ref.at[:, pl.ds(0, members * depth), lanes(slot)]

        def full(slot, member):
            return True if (slot + 1) * members <= tiles else slot * members + member < tiles

        def guarded(ok, body):
            if ok is True:
                body()
            else:
                pl.when(ok)(body)

        def block(slot, member):
            return w_ref.at[:, :, pl.ds(pl.multiple_of((slot * members + member) * LANES, LANES), LANES)]

        def spot(slot):
            return o_ref.at[:, pl.ds(pl.multiple_of(grid.me * depth, depth), depth), lanes(slot)]

        def out(slot, e):
            member = mine ^ e
            return remote(
                block(slot, member),
                spot(slot),
                send.at[slot, e],
                recv.at[slot],
                grid.where(member // 2, grid.column, member % 2),
            )

        def chunk(slot, r, column):
            return o_ref.at[:, pl.ds(pl.multiple_of((r * columns + column) * twice, twice), twice), lanes(slot)]

        def over(slot, r, e):
            here = chunk(slot, r, grid.column)
            return remote(
                here,
                here,
                push.at[slot, r, e],
                pull.at[slot, e],
                grid.where(grid.row, (grid.column + e) % columns, grid.core),
            )

        for slot in range(slots):
            for e in range(1, members):
                guarded(full(slot, mine ^ e), lambda: out(slot, e).start())
            guarded(
                full(slot, mine), lambda: pltpu.make_async_copy(block(slot, mine), spot(slot), recv.at[slot]).start()
            )
        last = slots - 1
        some = full(last, mine)
        if some is not True:
            fills = [
                pltpu.make_async_copy(zeros, o_ref.at[:, pl.ds(i * depth, depth), lanes(last)], blank.at[i])
                for i in range(count)
            ]

            @pl.when(jnp.logical_not(some))
            def _():
                zeros[...] = jnp.zeros_like(zeros)
                for fill in fills:
                    fill.start()
                for fill in fills:
                    fill.wait()

        yield True
        for slot in range(slots):

            def pass_on():
                pltpu.make_async_copy(bytes_of(slot), bytes_of(slot), recv.at[slot]).wait()
                for r in range(lines):
                    for e in range(1, columns):
                        over(slot, r, e).start()

            guarded(full(slot, mine), pass_on)
            yield True
        for slot in range(slots):

            def finish():
                for e in range(1, columns):
                    pltpu.make_async_copy(bytes_of(slot), bytes_of(slot), pull.at[slot, e]).wait()
                    for r in range(lines):
                        over(slot, r, e).wait_send()

            guarded(full(slot, mine), finish)
            for e in range(1, members):
                guarded(full(slot, mine ^ e), lambda: out(slot, e).wait_send())

    return Task(
        [w],
        [VMEM],
        [jax.ShapeDtypeStruct((kinds, count * depth, slots * LANES), w.dtype)],
        [HBM],
        [
            pltpu.VMEM((kinds, depth, LANES), w.dtype),
            dma((slots, members)),
            dma((slots,)),
            dma((slots, lines, columns)),
            dma((slots, columns)),
            dma((count,)),
        ],
        functools.partial(unit_targets, count),
        run,
    )


def collect(g, count, width):
    lines, columns = grid_of(count)
    kinds, rows, span = g.shape
    tiles = width // LANES
    members = 2 * lines
    slots = span // LANES
    depth = rows // count
    twice = 2 * depth

    def run(g_ref, o_ref, near, stage, push, pull, send, recv):
        grid = Grid(count)
        mine = grid.row * 2 + grid.core

        def lanes(slot):
            return pl.ds(slot * LANES, LANES)

        def guarded(slot, body):
            if (slot + 1) * members <= tiles:
                body()
            else:
                pl.when(slot * members + mine < tiles)(body)

        def rows_at(r, column):
            return pl.multiple_of((r * columns + column) * twice, twice)

        def over(slot, r, e):
            column = (grid.column + e) % columns
            return remote(
                g_ref.at[:, pl.ds(rows_at(r, column), twice), lanes(slot)],
                near.at[slot, e - 1, :, pl.ds(r * twice, twice)],
                push.at[slot, r, e],
                pull.at[slot, e],
                grid.where(grid.row, column, grid.core),
            )

        def spot(slot):
            return o_ref.at[:, :, pl.ds(pl.multiple_of((slot * members + mine) * LANES, LANES), LANES)]

        def piece(slot, member):
            return stage.at[slot, :, pl.ds(pl.multiple_of(member * depth, depth), depth)]

        def out(slot, e):
            member = mine ^ e
            return remote(
                piece(slot, member),
                spot(slot),
                send.at[slot, e],
                recv,
                grid.where(member // 2, grid.column, member % 2),
            )

        for slot in range(slots):

            def begin():
                for e in range(1, columns):
                    for r in range(lines):
                        over(slot, r, e).start()

            guarded(slot, begin)
        yield True
        for slot in range(slots):

            def add_up():
                for e in range(1, columns):
                    pltpu.make_async_copy(near.at[slot, e - 1], near.at[slot, e - 1], pull.at[slot, e]).wait()

                def add(i, carry):
                    for r in range(lines):
                        here = pl.ds(pl.multiple_of(rows_at(r, grid.column) + i * 16, 16), 16)
                        there = pl.ds(pl.multiple_of(r * twice + i * 16, 16), 16)
                        for kind in range(kinds):
                            value = g_ref[kind, here, lanes(slot)].astype(jnp.float32)
                            for e in range(1, columns):
                                value = value + near[slot, e - 1, kind, there].astype(jnp.float32)
                            stage[slot, kind, there] = value.astype(stage.dtype)
                    return carry

                lax.fori_loop(0, twice // 16, add, 0)
                for e in range(1, members):
                    out(slot, e).start()
                pltpu.make_async_copy(piece(slot, mine), spot(slot), recv).start()

            guarded(slot, add_up)
            yield True
        pltpu.make_async_copy(o_ref, o_ref, recv).wait()
        for slot in range(slots):

            def finish():
                for e in range(1, columns):
                    for r in range(lines):
                        over(slot, r, e).wait_send()
                for e in range(1, members):
                    out(slot, e).wait_send()

            guarded(slot, finish)

    return Task(
        [g],
        [VMEM],
        [jax.ShapeDtypeStruct((kinds, depth, width), g.dtype)],
        [VMEM],
        [
            pltpu.VMEM((slots, columns - 1, kinds, members * depth, LANES), g.dtype),
            pltpu.VMEM((slots, kinds, members * depth, LANES), g.dtype),
            dma((slots, lines, columns)),
            dma((slots, columns)),
            dma((slots, members)),
            dma,
        ],
        functools.partial(unit_targets, count),
        run,
    )


def window(most):
    def bounds(tokens):
        first = lax.axis_index("dp") * tokens
        return jnp.maximum(first - most + 1, 0) // KEYS, (first + tokens - 1) // KEYS + 1, first

    return bounds


def attend(most, begin, q, kv):
    tokens, heads = q.shape[0], q.shape[1] // HEAD_SIZE

    def run(begin_ref, q_ref, kv_ref, o_ref, lse_ref):
        low, high, first = window(most)(tokens)
        begin = begin_ref[...]
        index = first + lax.broadcasted_iota(jnp.int32, (tokens, 1), 0)
        lane = lax.broadcasted_iota(jnp.int32, (tokens, HEAD_SIZE), 1)
        key_lane = lax.broadcasted_iota(jnp.int32, (tokens, KEYS), 1)
        yield True
        for h in range(heads):
            cols = slice(h * HEAD_SIZE, (h + 1) * HEAD_SIZE)

            def step(block, state):
                top, mass, total = state
                start = pl.multiple_of(block * KEYS, KEYS)
                keys = kv_ref[pl.ds(start, KEYS), :HEAD_SIZE]
                values = kv_ref[pl.ds(start, KEYS), HEAD_SIZE:]
                scores = lax.dot_general(
                    q_ref[:, cols], keys, (((1,), (1,)), ((), ())), preferred_element_type=jnp.float32
                )
                at = key_lane + start
                scores = jnp.where((at >= begin) & (at <= index), scores * SCALE2, masked_score)
                best = jnp.maximum(top, jnp.max(scores, axis=1, keepdims=True))
                fade = jnp.exp2(top - best)
                probs = jnp.exp2(scores - best)
                mass = mass * fade + jnp.sum(probs, axis=1, keepdims=True)
                total = total * fade + jnp.dot(
                    probs.astype(jnp.bfloat16), values, preferred_element_type=jnp.float32
                )
                return best, mass, total

            top, mass, total = lax.fori_loop(
                low,
                high,
                step,
                (
                    jnp.full((tokens, 1), masked_score, jnp.float32),
                    jnp.zeros((tokens, 1), jnp.float32),
                    jnp.zeros((tokens, HEAD_SIZE), jnp.float32),
                ),
            )
            o_ref[:, cols] = total / mass
            lse = top + jnp.log2(mass)
            lse_ref[...] = jnp.where(lane == h, lse, 0.0 if h == 0 else lse_ref[...])
            yield True

    return Task(
        [begin, q, kv],
        [VMEM] * 3,
        [jax.ShapeDtypeStruct(q.shape, jnp.float32), jax.ShapeDtypeStruct((tokens, HEAD_SIZE), jnp.float32)],
        [VMEM] * 2,
        [],
        None,
        run,
    )


def forward(most, count, begin, q, kv, attn, x, gain):
    tokens, width = q.shape[0], x.shape[1]
    part, inner = x.shape[0], q.shape[1]
    core = attend(most, begin, q, kv)
    rows = gather(jax.ShapeDtypeStruct((part, width), jnp.bfloat16), count, tower=True)
    pair = swap([jax.ShapeDtypeStruct((part, width), jnp.bfloat16)])
    n_rows, n_pair = len(rows.scratch), len(pair.scratch)
    columns = 256
    skip = attn.shape[1] - inner

    def run(begin_ref, q_ref, kv_ref, attn_ref, x_ref, gain_ref, o_ref, lse_ref, hidden_ref, rows_ref, *scratch):
        sent, got, normed, whole = scratch[:4]
        half = lax.axis_index("head")
        yield from core.run(begin_ref, q_ref, kv_ref, o_ref, lse_ref)

        def project(i, carry):
            cols = pl.ds(pl.multiple_of(i * columns, columns), columns)
            whole[:, cols] = lax.dot_general(
                o_ref[...].astype(jnp.bfloat16),
                attn_ref[cols, skip:],
                (((1,), (1,)), ((), ())),
                preferred_element_type=jnp.float32,
            )
            return carry

        lax.fori_loop(0, width // columns, project, 0)

        def of(h):
            return pl.ds(pl.multiple_of(h * part, part), part)

        sent[...] = whole[of(1 - half)].astype(jnp.bfloat16)
        yield from pair.run(sent, got, *scratch[4 : 4 + n_pair])
        step = 16

        def norm(i, carry):
            here = pl.ds(pl.multiple_of(i * step, step), step)
            there = pl.ds(pl.multiple_of(half * part + i * step, step), step)
            hidden = x_ref[here].astype(jnp.float32) + (whole[there] + got[here].astype(jnp.float32))
            hidden_ref[here] = hidden
            normed[0, here] = (hidden * rms_scale(hidden) * gain_ref[...]).astype(jnp.bfloat16)
            return carry

        lax.fori_loop(0, part // step, norm, 0)
        yield from rows.run(normed, rows_ref, *scratch[4 + n_pair :])

    def targets():
        return pair.targets() + rows.targets()

    return Task(
        [begin, q, kv, attn, x, gain],
        [VMEM] * 6,
        core.outs + [jax.ShapeDtypeStruct((part, width), jnp.float32)] + rows.outs,
        [VMEM] * 3 + rows.out_specs,
        [
            pltpu.VMEM((part, width), jnp.bfloat16),
            pltpu.VMEM((part, width), jnp.bfloat16),
            pltpu.VMEM((1, part, width), jnp.bfloat16),
            pltpu.VMEM((tokens, width), jnp.float32),
        ]
        + pair.scratch
        + rows.scratch,
        targets,
        run,
    )


def attend_back(most, begin, q, kv, lse, raw, do):
    tokens, heads = q.shape[0], q.shape[1] // HEAD_SIZE
    across = (((1,), (1,)), ((), ()))
    down = (((0,), (0,)), ((), ()))

    def run(begin_ref, q_ref, kv_ref, lse_ref, raw_ref, do_ref, dq_ref, dkv_ref, delta_ref):
        low, high, first = window(most)(tokens)
        begin = begin_ref[...]
        index = first + lax.broadcasted_iota(jnp.int32, (tokens, 1), 0)
        lane = lax.broadcasted_iota(jnp.int32, (tokens, HEAD_SIZE), 1)
        key_lane = lax.broadcasted_iota(jnp.int32, (tokens, KEYS), 1)
        table = jnp.zeros((tokens, HEAD_SIZE), jnp.float32)
        for h in range(heads):
            cols = slice(h * HEAD_SIZE, (h + 1) * HEAD_SIZE)
            delta = jnp.sum(do_ref[:, cols].astype(jnp.float32) * raw_ref[:, cols], axis=1, keepdims=True)
            table = jnp.where(lane == h, delta, table)
        delta_ref[...] = table
        dq_ref[...] = jnp.zeros_like(dq_ref)
        blocks = kv_ref.shape[0] // KEYS

        def clear(block, carry):
            dkv_ref[block] = jnp.zeros((KEYS, 2 * HEAD_SIZE), dkv_ref.dtype)
            return carry

        lax.fori_loop(0, low, clear, 0)
        lax.fori_loop(high, blocks, clear, 0)

        def step(block, carry):
            start = pl.multiple_of(block * KEYS, KEYS)
            rows = pl.ds(start, KEYS)
            keys = kv_ref[rows, :HEAD_SIZE]
            values = kv_ref[rows, HEAD_SIZE:]
            at = key_lane + start
            seen = (at >= begin) & (at <= index)
            dk = jnp.zeros((KEYS, HEAD_SIZE), jnp.float32)
            dv = jnp.zeros((KEYS, HEAD_SIZE), jnp.float32)
            for h in range(heads):
                cols = slice(h * HEAD_SIZE, (h + 1) * HEAD_SIZE)
                q = q_ref[:, cols]
                do = do_ref[:, cols]
                scores = lax.dot_general(q, keys, across, preferred_element_type=jnp.float32)
                probs = jnp.where(seen, jnp.exp2(scores * SCALE2 - lse_ref[:, h : h + 1]), 0.0)
                pull = lax.dot_general(do, values, across, preferred_element_type=jnp.float32)
                ds = (probs * (pull - delta_ref[:, h : h + 1])).astype(jnp.bfloat16)
                dq_ref[:, cols] += jnp.dot(ds, keys, preferred_element_type=jnp.float32)
                dk = dk + lax.dot_general(ds, q, down, preferred_element_type=jnp.float32)
                dv = dv + lax.dot_general(
                    probs.astype(jnp.bfloat16), do, down, preferred_element_type=jnp.float32
                )
            dkv_ref[block, :, :HEAD_SIZE] = (dk * SCALE).astype(dkv_ref.dtype)
            dkv_ref[block, :, HEAD_SIZE:] = dv.astype(dkv_ref.dtype)
            return carry

        parts = 3
        reach = high - low
        yield True
        for i in range(parts):
            lax.fori_loop(low + reach * i // parts, low + reach * (i + 1) // parts, step, 0)
            yield True

    return Task(
        [begin, q, kv, lse, raw, do],
        [VMEM] * 6,
        [
            jax.ShapeDtypeStruct(q.shape, jnp.float32),
            jax.ShapeDtypeStruct((kv.shape[0] // KEYS, KEYS, kv.shape[1]), kv.dtype),
        ],
        [VMEM] * 2,
        [pltpu.VMEM((tokens, HEAD_SIZE), jnp.float32)],
        None,
        run,
    )


def doc_layout(row_lengths, first_token, token_count):
    doc_ends = jnp.cumsum(row_lengths)
    doc_starts = doc_ends - row_lengths
    token_index = first_token + jnp.arange(token_count, dtype=jnp.int32)
    doc_begin = jnp.max(
        jnp.where(doc_starts[None, :] <= token_index[:, None], doc_starts[None, :], 0), axis=1
    )
    return (doc_begin, token_index - doc_begin)


def rope_tables(positions):
    freq = rope_base ** (-jnp.arange(0, HEAD_SIZE, 2, dtype=jnp.float32) / HEAD_SIZE)
    angle = positions.astype(jnp.float32)[:, None] * freq[None, :]
    angle = jnp.concatenate([angle, angle], axis=1)
    return (jnp.cos(angle)[:, None, :], jnp.sin(angle)[:, None, :])


def rotary_apply(values, cosine_table, sine_table):
    half_width = values.shape[-1] // 2
    turned = jnp.concatenate([-values[..., half_width:], values[..., :half_width]], axis=-1)
    return values * cosine_table + turned * sine_table


def unrotate(grads, cosine_table, sine_table):
    half_width = grads.shape[-1] // 2
    scaled_grad = grads * sine_table
    back_part = jnp.concatenate(
        [scaled_grad[..., half_width:], -scaled_grad[..., :half_width]], axis=-1
    )
    return grads * cosine_table + back_part


def rms_scale(values):
    return lax.rsqrt(jnp.mean(values * values, axis=-1, keepdims=True) + norm_epsilon)


def norm_back(grad_out, inputs, scale, gain):
    weighted = grad_out * gain
    return scale * weighted - inputs * scale**3 * jnp.mean(
        weighted * inputs, axis=-1, keepdims=True
    )


def dot(a, b, dims=((1,), (0,))):
    return lax.dot_general(a, b, (dims, ((), ())), preferred_element_type=jnp.float32)


across_dims = ((1,), (1,))
token_dims = ((0,), (0,))


def backward(most, count, begin, q, kv, lse, raw, own, attn):
    tokens, width = q.shape[0], own.shape[1]
    part, inner = own.shape[0], q.shape[1]
    core = attend_back(most, begin, q, kv, lse, raw, jax.ShapeDtypeStruct(q.shape, jnp.bfloat16))
    d_query, d_kv = core.outs
    sums = scatter(jax.ShapeDtypeStruct((kv.shape[0], kv.shape[1]), kv.dtype), count)
    columns = 256
    skip = attn.shape[1] - inner

    def run(
        begin_ref, q_ref, kv_ref, lse_ref, raw_ref, own_ref, attn_ref, dq_ref, sums_ref, branch_ref, delta, do, dkv, send, recv, *scratch
    ):
        half = lax.axis_index("head")
        here = pl.ds(pl.multiple_of(half * part, part), part)
        copy = remote(
            own_ref, branch_ref.at[here], send, recv, {"dp": lax.axis_index("dp"), "head": 1 - half}
        )
        copy.start()
        branch_ref[here] = own_ref[...]
        yield True
        copy.wait_recv()

        def project(i, carry):
            cols = pl.ds(pl.multiple_of(i * columns, columns), columns)
            there = pl.ds(pl.multiple_of(skip + i * columns, columns), columns)
            do[:, cols] = jnp.dot(
                branch_ref[...], attn_ref[:, there], preferred_element_type=jnp.float32
            ).astype(do.dtype)
            return carry

        lax.fori_loop(0, inner // columns, project, 0)
        yield from core.run(begin_ref, q_ref, kv_ref, lse_ref, raw_ref, do, dq_ref, dkv, delta)
        yield from sums.run(dkv, sums_ref, *scratch)
        copy.wait_send()

    def targets():
        return [("half", True, {"dp": lax.axis_index("dp"), "head": 1 - lax.axis_index("head")})] + sums.targets()

    return Task(
        [begin, q, kv, lse, raw, own, attn],
        [VMEM] * 7,
        [d_query] + sums.outs + [jax.ShapeDtypeStruct((tokens, width), jnp.bfloat16)],
        [VMEM] * 3,
        core.scratch
        + [pltpu.VMEM(q.shape, jnp.bfloat16), pltpu.VMEM(d_kv.shape, d_kv.dtype), dma, dma]
        + sums.scratch,
        targets,
        run,
    )


def weight_grads(rows, grads, d_gate, d_up, active, weights):
    arrays = [rows, grads, d_gate, d_up, active, weights]
    width, units, tokens = rows.shape[1], active.shape[1], rows.shape[0]
    columns = 256
    down = (((0,), (0,)), ((), ()))
    across = (((1,), (1,)), ((), ()))

    def run(*refs):
        ins, (o_ref, out_ref), held, (sems,) = refs[:6], refs[6:8], refs[8:14], refs[14:]
        sources = list(ins[:5]) + [ins[5].at[2]]
        copies = [pltpu.make_async_copy(sources[i], held[i], sems.at[i]) for i in range(6)]
        for i in (4, 5, 0, 2, 3, 1):
            copies[i].start()
        yield True
        for i in (4, 5):
            copies[i].wait()

        def forth(i, carry):
            here = pl.ds(pl.multiple_of(i * columns, columns), columns)
            out_ref[here] = lax.dot_general(
                held[4][here], held[5][...], across, preferred_element_type=jnp.float32
            ).astype(out_ref.dtype)
            return carry

        lax.fori_loop(0, tokens // columns, forth, 0)
        yield True
        for i in (0, 2, 3):
            copies[i].wait()

        def first(i, carry):
            cols = pl.ds(pl.multiple_of(i * columns, columns), columns)
            for kind in (0, 1):
                o_ref[kind, cols] = lax.dot_general(
                    held[0][:, cols], held[2 + kind][...], down, preferred_element_type=jnp.float32
                ).astype(o_ref.dtype)
            return carry

        def second(i, carry):
            cols = pl.ds(pl.multiple_of(i * columns, columns), columns)
            o_ref[2, cols] = lax.dot_general(
                held[1][:, cols], held[4][...], down, preferred_element_type=jnp.float32
            ).astype(o_ref.dtype)
            return carry

        half = width // columns // 2
        lax.fori_loop(0, half, first, 0)
        yield True
        lax.fori_loop(half, width // columns, first, 0)
        yield True
        copies[1].wait()
        lax.fori_loop(0, width // columns, second, 0)
        yield True

    return Task(
        arrays,
        [HBM] * 6,
        [jax.ShapeDtypeStruct((3, width, units), jnp.bfloat16), jax.ShapeDtypeStruct((tokens, width), jnp.bfloat16)],
        [VMEM] * 2,
        [pltpu.VMEM(a.shape, a.dtype) for a in arrays[:5]] + [pltpu.VMEM((width, units), weights.dtype), dma((6,))],
        None,
        run,
    )


def longest(token_count):
    return 2048 if token_count == 4096 else token_count


def body(
    count,
    layer_in,
    gain_attn,
    q_weight,
    q_bias,
    key_weight,
    key_bias,
    value_weight,
    value_bias,
    o_weight,
    gain_mlp,
    gate_weight,
    up_weight,
    down_weight,
    row_lengths,
    source_ids,
    source_weights,
    out_grad,
):
    f32, bf16 = jnp.float32, jnp.bfloat16
    tok_rows, width = layer_in.shape
    part = tok_rows // 2
    half = lax.axis_index("head")
    first_token = lax.axis_index("dp") * tok_rows
    doc_begin, positions = doc_layout(row_lengths, first_token, tok_rows)
    cosine_table, sine_table = rope_tables(positions)
    q_cols = q_weight.shape[1]
    kv_cols = key_weight.shape[1]
    heads = q_cols // HEAD_SIZE
    ff_cols = gate_weight.shape[1]

    def mine(rows):
        return lax.dynamic_slice_in_dim(rows, half * part, part, 0)

    def other(rows):
        return lax.dynamic_slice_in_dim(rows, (1 - half) * part, part, 0)

    def join(own, peer):
        return jnp.where(half == 0, jnp.concatenate([own, peer]), jnp.concatenate([peer, own]))

    attn_local = jnp.concatenate([q_weight, key_weight, value_weight, o_weight.T], axis=1)
    picked = source_ids[:, None] == jnp.arange(source_weights.shape[0], dtype=jnp.int32)[None, :]
    row_scale = (
        jnp.sum(jnp.where(picked, source_weights[None, :], 0), axis=1).astype(f32) / loss_denominator
    )
    cotangent = mine(out_grad).astype(f32) * mine(row_scale[:, None])
    ((attn_full,),) = fuse(1, "gather_weights", gather(attn_local, count))
    attn_full = attn_full.reshape(width, -1)
    qkv_cols = q_cols + 2 * kv_cols
    full_qkv = attn_full[:, :qkv_cols]
    full_o = attn_full[:, qkv_cols:]
    inputs = layer_in.astype(f32)
    scale_one = rms_scale(inputs)
    gain_one = gain_attn.astype(f32)
    normed = (inputs * scale_one * gain_one).astype(bf16)
    bias = jnp.concatenate([q_bias, key_bias, value_bias]).astype(f32)
    pre = dot(normed, full_qkv) + bias
    turned = rotary_apply(
        pre[:, : q_cols + kv_cols].reshape(tok_rows, heads + 1, HEAD_SIZE), cosine_table, sine_table
    ).reshape(tok_rows, q_cols + kv_cols)
    query_rows = turned[:, :q_cols].astype(bf16)
    kv_rows = jnp.concatenate([turned[:, q_cols:], pre[:, q_cols + kv_cols :]], axis=1).astype(bf16)
    ((kv_all,), (grad_all,)) = fuse(
        2, "gather_keys", gather(kv_rows, count), gather(cotangent.astype(bf16), count, tower=True)
    )
    grad_all = grad_all.reshape(-1, width)
    kv_all = kv_all.reshape(-1, 2 * kv_cols)
    begin = doc_begin[:, None].astype(jnp.int32)
    most = longest(count * tok_rows)
    mlp_local = jnp.stack([gate_weight, up_weight, down_weight.T])
    gain_two = gain_mlp.astype(f32)
    ahead = (0, 1) + (1, 1, 1, 0) + (1, 1, 1, 0) + (1, 0, 1, 1, 0) + (1,) * 6 + (0,)
    ((mlp_full,), (attended_raw, row_lse, hidden, rows_all)) = fuse(
        3,
        "forward_spread",
        spread(mlp_local, count),
        forward(most, count, begin, query_rows, kv_all, attn_full, mine(layer_in), gain_two[None, :]),
        order=ahead,
    )
    attended = attended_raw.astype(bf16)
    scale_two = rms_scale(hidden)
    rows_all = rows_all.reshape(-1, width)

    full_gate, full_up, full_down = mlp_full[0], mlp_full[1], mlp_full[2]
    gate_act = dot(rows_all, full_gate)
    up_act = dot(rows_all, full_up)
    sigmoid_gate = jax.nn.sigmoid(gate_act)
    silu_gate = gate_act * sigmoid_gate
    active = (silu_gate * up_act).astype(bf16)
    d_active = dot(grad_all, full_down)
    d_gate = (d_active * up_act * sigmoid_gate * (1.0 + gate_act * (1.0 - sigmoid_gate))).astype(bf16)
    d_up = (d_active * silu_gate).astype(bf16)
    norm_two_part = (dot(d_gate, full_gate, across_dims) + dot(d_up, full_up, across_dims)).astype(bf16)

    if count <= 16:
        ((d_normed_mlp,), (mlp_grads, mlp_part)) = fuse(
            8,
            "scatter_grads",
            scatter(norm_two_part, count, tower=True),
            weight_grads(rows_all, grad_all, d_gate, d_up, active, mlp_full),
            order=(0, 1, 0, 0, 1, 0, 0, 1, 0, 1, 0, 1),
        )
    else:
        d_normed_mlp = scatter_all(norm_two_part, count, 8, "scatter_rows", tower=True)
        mlp_part = dot(active, full_down, across_dims).astype(bf16)
        mlp_grads = jnp.stack(
            [
                dot(rows_all, d_gate, token_dims).astype(bf16),
                dot(rows_all, d_up, token_dims).astype(bf16),
                dot(grad_all, active, token_dims).astype(bf16),
            ]
        )
    gain_two_local = jnp.sum(d_normed_mlp * hidden * scale_two, axis=0)
    d_hidden = cotangent + norm_back(d_normed_mlp, hidden, scale_two, gain_two)
    branch_own = d_hidden.astype(bf16)
    tasks = [
        collect(mlp_grads, count, ff_cols),
        backward(most, count, begin, query_rows, kv_all, row_lse, attended_raw, branch_own, attn_full),
    ]
    turns = (1, 0, 1, 1, 0, 1, 0, 1, 0, 1, 1, 0)
    if count <= 16:
        tasks.append(scatter(mlp_part, count, tower=True))
        turns = (1, 0) + (2,) * 5 + (1, 0, 1, 2, 0, 1, 2, 0, 1, 2, 0, 1) + (1,) * 4 + (0, 2)
    found = fuse(17, "backward_collect", *tasks, order=turns)
    ((mlp_part_sums,), (d_query, kv_sums, branch_grad)) = found[:2]
    mlp_out = found[2][0] if count <= 16 else scatter_all(mlp_part, count, 25, "scatter_out", tower=True)
    layer_out_own = (hidden + mlp_out).astype(bf16)
    mlp_part_sums = mlp_part_sums.astype(f32)
    out_proj_grad = dot(branch_grad, attended, token_dims)
    d_queries = (d_query * SCALE).astype(bf16).astype(f32)
    d_key_rot = kv_sums[:, :kv_cols].astype(bf16).astype(f32)
    d_value_rows = kv_sums[:, kv_cols:].astype(bf16)
    d_turned = jnp.concatenate([d_queries, d_key_rot], axis=1).reshape(tok_rows, heads + 1, HEAD_SIZE)
    d_pre = jnp.concatenate(
        [
            unrotate(d_turned, cosine_table, sine_table).reshape(tok_rows, q_cols + kv_cols).astype(bf16),
            d_value_rows,
        ],
        axis=1,
    )
    bias_local = jnp.sum(d_pre.astype(f32), axis=0)
    qkv_grad = dot(normed, d_pre, token_dims)
    attn_grads = jnp.concatenate([qkv_grad, out_proj_grad], axis=1).astype(bf16)
    norm_one_part = dot(d_pre, full_qkv, across_dims)
    norm_send = other(norm_one_part).astype(bf16)
    exchange = swap([norm_send, layer_out_own])
    if count <= 16:
        ((attn_part,), (norm_peer, layer_out_peer)) = fuse(21, "scatter_last", scatter(attn_grads, count), exchange)
    else:
        attn_part = scatter_all(attn_grads, count, 21, "scatter_attn")
        ((norm_peer, layer_out_peer),) = fuse(33, "swap_norm", exchange)
    d_normed = mine(norm_one_part) + norm_peer.astype(f32)
    inputs_own = mine(inputs)
    scale_own = mine(scale_one)
    gain_one_local = jnp.sum(d_normed * inputs_own * scale_own, axis=0)
    layer_in_grad_own = (d_hidden + norm_back(d_normed, inputs_own, scale_own, gain_one)).astype(bf16)

    small = jnp.concatenate([bias_local, gain_one_local, gain_two_local]).reshape(-1, LANES)
    ((small_all,), (layer_in_grad_peer,)) = fuse(
        34, "gather_sums", gather(small, count, both=True), swap([layer_in_grad_own])
    )
    small_all = small_all.reshape(count, 2, -1)
    small_sum = jnp.sum(small_all[:, 0], axis=0)
    gains = (small_sum[qkv_cols:] + jnp.sum(small_all[:, 1, qkv_cols:], axis=0)).reshape(2, width)
    layer_in_grad = join(layer_in_grad_own, layer_in_grad_peer)
    layer_out = join(layer_out_own, layer_out_peer)
    return (
        layer_out,
        layer_in_grad,
        gains[0],
        attn_part[:, :q_cols],
        small_sum[:q_cols],
        attn_part[:, q_cols : q_cols + kv_cols],
        small_sum[q_cols : q_cols + kv_cols],
        attn_part[:, q_cols + kv_cols : qkv_cols],
        small_sum[q_cols + kv_cols : qkv_cols],
        attn_part[:, qkv_cols:].T,
        gains[1],
        mlp_part_sums[0],
        mlp_part_sums[1],
        mlp_part_sums[2].T,
    )


def solution(mesh):
    placed = (
        P("dp", None),
        P(),
        P("dp", "head"),
        P("head"),
        P("dp", "head"),
        P("head"),
        P("dp", "head"),
        P("head"),
        P("head", "dp"),
        P(),
        P("dp", "head"),
        P("dp", "head"),
        P("head", "dp"),
        P(),
        P("dp"),
        P(),
        P("dp", None),
    )
    return jax.shard_map(
        functools.partial(body, mesh.shape["dp"]),
        mesh=mesh,
        in_specs=placed,
        out_specs=(
            P("dp", None),
            P("dp", None),
            P(),
            P("dp", "head"),
            P("head"),
            P("dp", "head"),
            P("head"),
            P("dp", "head"),
            P("head"),
            P("head", "dp"),
            P(),
            P("dp", "head"),
            P("dp", "head"),
            P("head", "dp"),
        ),
        check_vma=False,
    )
```

```python
import dataclasses
import functools
from typing import Any, Callable
import jax
import jax.numpy as jnp
from jax import lax
from jax.experimental import pallas as pl
from jax.experimental.pallas import tpu as pltpu
from jax.sharding import PartitionSpec as P

HEAD_SIZE = 128
KEYS = 256
SCALE = HEAD_SIZE**-0.5
SCALE2 = SCALE * 1.4426950408889634
MESH = pl.DeviceIdType.MESH
LANES = 128
norm_epsilon = 1e-06
rope_base = 1000000.0
loss_denominator = 16.0
masked_score = -1e30
VMEM = pl.BlockSpec(memory_space=pltpu.VMEM)
HBM = pl.BlockSpec(memory_space=pl.ANY)
dma = pltpu.SemaphoreType.DMA


def grid_of(count):
    across = 2 if count <= 16 else 4
    return count // (2 * across), across


def remote(src, dst, send, recv, where):
    return pltpu.make_async_remote_copy(
        src_ref=src, dst_ref=dst, send_sem=send, recv_sem=recv, device_id=where, device_id_type=MESH
    )


def reshape(x, shape):
    if isinstance(x, jax.ShapeDtypeStruct):
        return jax.ShapeDtypeStruct(shape, x.dtype)
    return x.reshape(shape)


class Grid:
    def __init__(self, count, tower=False):
        self.lines, self.columns = grid_of(count)
        self.tower = tower
        self.across = 2 if tower else self.columns
        me, self.half = lax.axis_index("dp"), lax.axis_index("head")
        self.me = me
        self.core = me % 2
        self.column = (me // 2) % self.columns
        self.row = me // (2 * self.columns)
        self.col = self.half if tower else self.column

    def where(self, r, q, k):
        if self.tower:
            return {"dp": (r * self.columns + self.column) * 2 + k, "head": q}
        return {"dp": (r * self.columns + q) * 2 + k, "head": self.half}

    def index(self, r, q, k):
        return (r * self.across + q) * 2 + k


@dataclasses.dataclass
class Task:
    inputs: list
    in_specs: list
    outs: list
    out_specs: list
    scratch: list
    targets: Callable
    run: Callable


def fuse(ident, name, *tasks, order=()):
    remote_ops = any(t.targets is not None for t in tasks)

    def split(refs, sizes):
        parts, start = [], 0
        for size in sizes:
            parts.append(refs[start : start + size])
            start += size
        return parts

    n_in = [len(t.inputs) for t in tasks]
    n_out = [len(t.outs) for t in tasks]
    n_scratch = [len(t.scratch) for t in tasks]

    def kernel(*refs):
        ins, outs, scratch = split(refs, [sum(n_in), sum(n_out), sum(n_scratch)])
        if remote_ops:
            barrier = pltpu.get_barrier_semaphore()
            known, total = set(), 0
            for t in tasks:
                for key, ok, where in t.targets() if t.targets is not None else ():
                    if key in known:
                        continue
                    known.add(key)
                    if ok is True:
                        pl.semaphore_signal(barrier, inc=1, device_id=where, device_id_type=MESH)
                        total = total + 1
                    else:

                        @pl.when(ok)
                        def _():
                            pl.semaphore_signal(barrier, inc=1, device_id=where, device_id_type=MESH)

                        total = total + ok.astype(jnp.int32)
            pl.semaphore_wait(barrier, total)
        steps = [
            t.run(*a, *b, *c)
            for t, a, b, c in zip(tasks, split(ins, n_in), split(outs, n_out), split(scratch, n_scratch))
        ]
        live = set(range(len(steps)))
        turns = list(order)
        while live:
            for i in turns:
                if i in live and next(steps[i], None) is None:
                    live.remove(i)
            turns = sorted(live)

    params = dict(vmem_limit_bytes=60 << 20)
    if remote_ops:
        params.update(collective_id=ident, has_side_effects=True)
    flat = pl.pallas_call(
        kernel,
        out_shape=[o for t in tasks for o in t.outs],
        in_specs=[s for t in tasks for s in t.in_specs],
        out_specs=[s for t in tasks for s in t.out_specs],
        scratch_shapes=[s for t in tasks for s in t.scratch],
        compiler_params=pltpu.CompilerParams(**params),
        name=name,
    )(*[x for t in tasks for x in t.inputs])
    return split(flat, n_out)


def gather(x, count, tower=False, pieces=1, both=False, flat=False):
    lines, columns = grid_of(count)
    across = 2 if tower else columns
    members = lines * across * 2
    shape = x.shape
    pieces = 1 if both else pieces
    x = reshape(x, (pieces, shape[0] // pieces) + shape[1:])
    copies = 2 if both else pieces

    def hops_of(grid):
        row, col, core = grid.row, grid.col, grid.core
        return (
            (row < lines - 1, grid.where(row + 1, col, core)),
            (row > 0, grid.where(row - 1, col, core)),
            (col < across - 1, grid.where(row, col + 1, core)),
            (col > 0, grid.where(row, col - 1, core)),
            (True, grid.where(row, col, 1 - core)),
        )

    def targets():
        grid = Grid(count, tower)
        found = [(("hop", tower, i), ok, to) for i, (ok, to) in enumerate(hops_of(grid))]
        if both:
            found.append(("half", True, {"dp": grid.me, "head": 1 - grid.half}))
        return found

    def run(x_ref, o_ref, send, recv, local, cross):
        grid = Grid(count, tower)
        hops = hops_of(grid)
        core, col, row = grid.core, grid.col, grid.row
        me = grid.index(row, col, core)

        def spot(shard, piece):
            if flat:
                return o_ref.at[pl.ds(pl.multiple_of(shard * shape[0], shape[0]), shape[0])]
            return o_ref.at[shard, piece]

        def copy(hop, shard, piece, src):
            return remote(src, spot(shard, piece), send.at[hop, shard, piece], recv.at[shard, piece], hops[hop][1])

        order = sorted(
            ((dr, dq) for dr in range(1 - lines, lines) for dq in range(1 - across, across)),
            key=lambda p: (abs(p[0]) + abs(p[1]), abs(p[1])),
        )
        if both:
            pair = remote(
                x_ref.at[0], o_ref.at[me, 1], cross.at[0], cross.at[1], {"dp": grid.me, "head": 1 - grid.half}
            )
            pair.start()
        sends = []
        mine = pltpu.make_async_copy(
            x_ref.at[0] if flat else x_ref, spot(me, 0) if flat else o_ref.at[me, pl.ds(0, pieces)], local
        )
        for dr, dq in order:
            shard = grid.index(row - dr, col - dq, core)
            valid = (row - dr >= 0) & (row - dr < lines) & (col - dq >= 0) & (col - dq < across)
            onward = []
            if dq == 0:
                if dr >= 0:
                    onward.append(0)
                if dr <= 0:
                    onward.append(1)
            if dq >= 0:
                onward.append(2)
            if dq <= 0:
                onward.append(3)
            onward.append(4)
            for piece in range(copies):
                own = dr == 0 and dq == 0
                src = spot(shard, piece)
                if own and piece < pieces:
                    src = x_ref.at[piece]
                if own and piece >= pieces:
                    pair.wait_recv()
                if not own:

                    @pl.when(valid)
                    def _():
                        copy(4, shard, piece, src).wait_recv()

                for hop in onward:
                    ok = hops[hop][0]
                    go = valid if ok is True else valid & ok

                    @pl.when(go)
                    def _():
                        copy(hop, shard, piece, src).start()

                    sends.append((go, hop, shard, piece, src))
                yield True
            if dr == 0 and dq == 0:
                mine.start()
        for r in range(lines):
            for q in range(across):
                for piece in range(copies):
                    shard = grid.index(r, q, 1 - core)
                    copy(4, shard, piece, spot(shard, piece)).wait_recv()
        yield True
        for go, hop, shard, piece, src in sends:

            @pl.when(go)
            def _():
                copy(hop, shard, piece, src).wait_send()

        mine.wait()
        if both:
            pair.wait_send()

    return Task(
        [x],
        [VMEM],
        [jax.ShapeDtypeStruct((members * shape[0],) + shape[1:] if flat else (members, copies) + x.shape[1:], x.dtype)],
        [VMEM if flat else HBM],
        [dma((5, members, copies)), dma((members, copies)), dma, dma((2,))],
        targets,
        run,
    )


def scatter(x, count, tower=False, dtype=jnp.float32):
    lines, columns = grid_of(count)
    across = 2 if tower else columns
    members = lines * across * 2
    block = (x.shape[0] // members,) + x.shape[1:]
    height = block[0]
    step = 16
    x = reshape(x, (members,) + block)

    def targets():
        grid = Grid(count, tower)
        row, col, core = grid.row, grid.col, grid.core
        found = [(("hop", tower, 4), True, grid.where(row, col, 1 - core))]
        found += [(("col", tower, e), True, grid.where(row, (col + e) % across, core)) for e in range(1, across)]
        found.append((("hop", tower, 0), row < lines - 1, grid.where(row + 1, col, core)))
        found.append((("hop", tower, 1), row > 0, grid.where(row - 1, col, core)))
        return found

    def run(x_ref, o_ref, near, first, wide, second, far, s1, r1, s2, r2, s3, r3):
        grid = Grid(count, tower)
        row, col, core = grid.row, grid.col, grid.core

        def one(r, q):
            return remote(
                x_ref.at[grid.index(r, q, 1 - core)], near.at[r, q], s1.at[r, q], r1.at[r, q], grid.where(row, col, 1 - core)
            )

        def two(r, e):
            return remote(
                first.at[r, e - 1], wide.at[r, e - 1], s2.at[r, e], r2.at[r, e], grid.where(row, (col + e) % across, core)
            )

        def three(r):
            to = jnp.where(r > row, row + 1, row - 1)
            place = jnp.where((r > row) | (to != r), r, lines)
            return remote(second.at[r], far.at[place], s3.at[r], r3.at[place], grid.where(to, col, core))

        def arrived(place):
            remote(second.at[0], far.at[place], s3.at[0], r3.at[place], grid.where(row, col, 1 - core)).wait_recv()

        def turn(t):
            return jnp.where(row < lines // 2, lines - 1 - t, t)

        for t in range(lines):
            r = turn(t)
            for e in [e for e in range(1, across)] + [0]:
                one(r, (col + e) % across).start()
        yield True

        def blocks(body):
            def run_block(i, carry):
                body(pl.ds(pl.multiple_of(i * step, step), step))
                return carry

            lax.fori_loop(0, height // step, run_block, 0)

        for t in range(lines):
            r = turn(t)
            for e in range(1, across):
                q = (col + e) % across
                one(r, q).wait_recv()

                def add(rows):
                    first[r, e - 1, rows] = (
                        x_ref[grid.index(r, q, core), rows].astype(jnp.float32) + near[r, q, rows].astype(jnp.float32)
                    ).astype(first.dtype)

                blocks(add)
                two(r, e).start()
            yield True
        for t in range(lines):
            r = turn(t)
            one(r, col).wait_recv()
            for e in range(1, across):
                two(r, e).wait_recv()
            behind = ((r > row) & (row > 0)) | ((r < row) & (row < lines - 1))

            def total(rows):
                value = x_ref[grid.index(r, col, core), rows].astype(jnp.float32) + near[r, col, rows].astype(jnp.float32)
                for e in range(1, across):
                    value = value + wide[r, e - 1, rows].astype(jnp.float32)
                return value

            @pl.when(r == row)
            def _():
                def keep(rows):
                    o_ref[rows] = total(rows).astype(o_ref.dtype)

                blocks(keep)

            @pl.when((r != row) & jnp.logical_not(behind))
            def _():
                def begin(rows):
                    second[r, rows] = total(rows).astype(second.dtype)

                blocks(begin)
                three(r).start()

            @pl.when((r != row) & behind)
            def _():
                arrived(r)

                def pass_on(rows):
                    second[r, rows] = (total(rows) + far[r, rows].astype(jnp.float32)).astype(second.dtype)

                blocks(pass_on)
                three(r).start()

            yield True
        for ok, place in ((row > 0, row), (row < lines - 1, lines)):

            @pl.when(ok)
            def _():
                arrived(place)

                def last(rows):
                    o_ref[rows] = (o_ref[rows] + far[place, rows].astype(jnp.float32)).astype(o_ref.dtype)

                blocks(last)

        yield True
        for r in range(lines):
            for q in range(across):
                one(r, q).wait_send()
            for e in range(1, across):
                two(r, e).wait_send()

            @pl.when(r != row)
            def _():
                three(r).wait_send()

    return Task(
        [x],
        [VMEM],
        [jax.ShapeDtypeStruct(block, dtype)],
        [VMEM],
        [
            pltpu.VMEM((lines, across) + block, x.dtype),
            pltpu.VMEM((lines, across - 1) + block, x.dtype),
            pltpu.VMEM((lines, across - 1) + block, x.dtype),
            pltpu.VMEM((lines,) + block, x.dtype),
            pltpu.VMEM((lines + 1,) + block, x.dtype),
            dma((lines, across)),
            dma((lines, across)),
            dma((lines, across)),
            dma((lines, across)),
            dma((lines,)),
            dma((lines + 1,)),
        ],
        targets,
        run,
    )


def scatter_all(x, count, ident, name, **how):
    cuts = max(1, x.size * x.dtype.itemsize >> 23)
    span = x.shape[1] // cuts
    parts = [
        fuse(ident + i, f"{name}{i}", scatter(x[:, i * span : (i + 1) * span], count, **how))[0][0] for i in range(cuts)
    ]
    return parts[0] if cuts == 1 else jnp.concatenate(parts, axis=1)


def swap(arrays):
    parts = len(arrays)

    def targets():
        return [("half", True, {"dp": lax.axis_index("dp"), "head": 1 - lax.axis_index("head")})]

    def run(*refs):
        ins, outs = refs[:parts], refs[parts : 2 * parts]
        send, recv = refs[2 * parts :]
        where = targets()[0][2]
        copies = [remote(ins[i], outs[i], send.at[i], recv.at[i], where) for i in range(parts)]
        for copy in copies:
            copy.start()
        yield True
        for copy in copies:
            copy.wait()

    return Task(
        list(arrays),
        [VMEM] * parts,
        [jax.ShapeDtypeStruct(a.shape, a.dtype) for a in arrays],
        [VMEM] * parts,
        [dma((parts,)), dma((parts,))],
        targets,
        run,
    )


def unit_targets(count):
    lines, columns = grid_of(count)
    grid = Grid(count)
    mine = grid.row * 2 + grid.core
    found = []
    for e in range(1, 2 * lines):
        member = mine ^ e
        found.append((("member", e), True, grid.where(member // 2, grid.column, member % 2)))
    for e in range(1, columns):
        found.append((("col", False, e), True, grid.where(grid.row, (grid.column + e) % columns, grid.core)))
    return found


def spread(w, count):
    lines, columns = grid_of(count)
    kinds, depth, width = w.shape
    tiles = width // LANES
    members = 2 * lines
    slots = pl.cdiv(tiles, members)
    twice = 2 * depth

    def run(w_ref, o_ref, zeros, send, recv, push, pull, blank):
        grid = Grid(count)
        mine = grid.row * 2 + grid.core

        def lanes(slot):
            return pl.ds(slot * LANES, LANES)

        def bytes_of(slot):
            return o_ref.at[:, pl.ds(0, members * depth), lanes(slot)]

        def full(slot, member):
            return True if (slot + 1) * members <= tiles else slot * members + member < tiles

        def guarded(ok, body):
            if ok is True:
                body()
            else:
                pl.when(ok)(body)

        def block(slot, member):
            return w_ref.at[:, :, pl.ds(pl.multiple_of((slot * members + member) * LANES, LANES), LANES)]

        def spot(slot):
            return o_ref.at[:, pl.ds(pl.multiple_of(grid.me * depth, depth), depth), lanes(slot)]

        def out(slot, e):
            member = mine ^ e
            return remote(
                block(slot, member),
                spot(slot),
                send.at[slot, e],
                recv.at[slot],
                grid.where(member // 2, grid.column, member % 2),
            )

        def chunk(slot, r, column):
            return o_ref.at[:, pl.ds(pl.multiple_of((r * columns + column) * twice, twice), twice), lanes(slot)]

        def over(slot, r, e):
            here = chunk(slot, r, grid.column)
            return remote(
                here,
                here,
                push.at[slot, r, e],
                pull.at[slot, e],
                grid.where(grid.row, (grid.column + e) % columns, grid.core),
            )

        def begin(slot):
            for e in range(1, members):
                guarded(full(slot, mine ^ e), lambda: out(slot, e).start())
            guarded(
                full(slot, mine), lambda: pltpu.make_async_copy(block(slot, mine), spot(slot), recv.at[slot]).start()
            )

        last = slots - 1
        some = full(last, mine)
        if some is not True:
            fills = [
                pltpu.make_async_copy(zeros, o_ref.at[:, pl.ds(i * depth, depth), lanes(last)], blank.at[i])
                for i in range(count)
            ]

            @pl.when(jnp.logical_not(some))
            def _():
                zeros[...] = jnp.zeros_like(zeros)
                for fill in fills:
                    fill.start()
                for fill in fills:
                    fill.wait()

        def relay(slot):
            def pass_on():
                pltpu.make_async_copy(bytes_of(slot), bytes_of(slot), recv.at[slot]).wait()
                for r in range(lines):
                    for e in range(1, columns):
                        over(slot, r, e).start()

            guarded(full(slot, mine), pass_on)

        lead = min(3, slots)
        for slot in range(lead):
            begin(slot)
            yield True
        for slot in range(slots):
            relay(slot)
            yield True
            if slot + lead < slots:
                begin(slot + lead)
                yield True
        for slot in range(slots):

            def finish():
                for e in range(1, columns):
                    pltpu.make_async_copy(bytes_of(slot), bytes_of(slot), pull.at[slot, e]).wait()
                    for r in range(lines):
                        over(slot, r, e).wait_send()

            guarded(full(slot, mine), finish)
            for e in range(1, members):
                guarded(full(slot, mine ^ e), lambda: out(slot, e).wait_send())

    return Task(
        [w],
        [VMEM],
        [jax.ShapeDtypeStruct((kinds, count * depth, slots * LANES), w.dtype)],
        [HBM],
        [
            pltpu.VMEM((kinds, depth, LANES), w.dtype),
            dma((slots, members)),
            dma((slots,)),
            dma((slots, lines, columns)),
            dma((slots, columns)),
            dma((count,)),
        ],
        functools.partial(unit_targets, count),
        run,
    )


def collect(g, count, width):
    lines, columns = grid_of(count)
    kinds, rows, span = g.shape
    tiles = width // LANES
    members = 2 * lines
    slots = span // LANES
    depth = rows // count
    twice = 2 * depth

    def run(g_ref, o_ref, near, stage, push, pull, send, recv):
        grid = Grid(count)
        mine = grid.row * 2 + grid.core

        def lanes(slot):
            return pl.ds(slot * LANES, LANES)

        def guarded(slot, body):
            if (slot + 1) * members <= tiles:
                body()
            else:
                pl.when(slot * members + mine < tiles)(body)

        def rows_at(r, column):
            return pl.multiple_of((r * columns + column) * twice, twice)

        def over(slot, r, e):
            column = (grid.column + e) % columns
            return remote(
                g_ref.at[:, pl.ds(rows_at(r, column), twice), lanes(slot)],
                near.at[slot, e - 1, :, pl.ds(r * twice, twice)],
                push.at[slot, r, e],
                pull.at[slot, e],
                grid.where(grid.row, column, grid.core),
            )

        def spot(slot):
            return o_ref.at[:, :, pl.ds(pl.multiple_of((slot * members + mine) * LANES, LANES), LANES)]

        def piece(slot, member):
            return stage.at[slot, :, pl.ds(pl.multiple_of(member * depth, depth), depth)]

        def out(slot, e):
            member = mine ^ e
            return remote(
                piece(slot, member),
                spot(slot),
                send.at[slot, e],
                recv,
                grid.where(member // 2, grid.column, member % 2),
            )

        for slot in range(slots):

            def begin():
                for e in range(1, columns):
                    for r in range(lines):
                        over(slot, r, e).start()

            guarded(slot, begin)
        yield True
        for slot in range(slots):

            def add_up():
                for e in range(1, columns):
                    pltpu.make_async_copy(near.at[slot, e - 1], near.at[slot, e - 1], pull.at[slot, e]).wait()

                def add(i, carry):
                    for r in range(lines):
                        here = pl.ds(pl.multiple_of(rows_at(r, grid.column) + i * 16, 16), 16)
                        there = pl.ds(pl.multiple_of(r * twice + i * 16, 16), 16)
                        for kind in range(kinds):
                            value = g_ref[kind, here, lanes(slot)].astype(jnp.float32)
                            for e in range(1, columns):
                                value = value + near[slot, e - 1, kind, there].astype(jnp.float32)
                            stage[slot, kind, there] = value.astype(stage.dtype)
                    return carry

                lax.fori_loop(0, twice // 16, add, 0)
                for e in range(1, members):
                    out(slot, e).start()
                pltpu.make_async_copy(piece(slot, mine), spot(slot), recv).start()

            guarded(slot, add_up)
            yield True
        pltpu.make_async_copy(o_ref, o_ref, recv).wait()
        for slot in range(slots):

            def finish():
                for e in range(1, columns):
                    for r in range(lines):
                        over(slot, r, e).wait_send()
                for e in range(1, members):
                    out(slot, e).wait_send()

            guarded(slot, finish)

    return Task(
        [g],
        [VMEM],
        [jax.ShapeDtypeStruct((kinds, depth, width), g.dtype)],
        [VMEM],
        [
            pltpu.VMEM((slots, columns - 1, kinds, members * depth, LANES), g.dtype),
            pltpu.VMEM((slots, kinds, members * depth, LANES), g.dtype),
            dma((slots, lines, columns)),
            dma((slots, columns)),
            dma((slots, members)),
            dma,
        ],
        functools.partial(unit_targets, count),
        run,
    )


def window(most):
    def bounds(tokens):
        first = lax.axis_index("dp") * tokens
        return jnp.maximum(first - most + 1, 0) // KEYS, (first + tokens - 1) // KEYS + 1, first

    return bounds


def attend(most, begin, q, kv):
    tokens, heads = q.shape[0], q.shape[1] // HEAD_SIZE

    def run(begin_ref, q_ref, kv_ref, o_ref, lse_ref):
        low, high, first = window(most)(tokens)
        begin = begin_ref[...]
        index = first + lax.broadcasted_iota(jnp.int32, (tokens, 1), 0)
        lane = lax.broadcasted_iota(jnp.int32, (tokens, HEAD_SIZE), 1)
        key_lane = lax.broadcasted_iota(jnp.int32, (tokens, KEYS), 1)
        yield True
        for h in range(heads):
            cols = slice(h * HEAD_SIZE, (h + 1) * HEAD_SIZE)

            def step(block, state):
                top, mass, total = state
                start = pl.multiple_of(block * KEYS, KEYS)
                keys = kv_ref[pl.ds(start, KEYS), :HEAD_SIZE]
                values = kv_ref[pl.ds(start, KEYS), HEAD_SIZE:]
                scores = lax.dot_general(
                    q_ref[:, cols], keys, (((1,), (1,)), ((), ())), preferred_element_type=jnp.float32
                )
                at = key_lane + start
                scores = jnp.where((at >= begin) & (at <= index), scores * SCALE2, masked_score)
                best = jnp.maximum(top, jnp.max(scores, axis=1, keepdims=True))
                fade = jnp.exp2(top - best)
                probs = jnp.exp2(scores - best)
                mass = mass * fade + jnp.sum(probs, axis=1, keepdims=True)
                total = total * fade + jnp.dot(
                    probs.astype(jnp.bfloat16), values, preferred_element_type=jnp.float32
                )
                return best, mass, total

            top, mass, total = lax.fori_loop(
                low,
                high,
                step,
                (
                    jnp.full((tokens, 1), masked_score, jnp.float32),
                    jnp.zeros((tokens, 1), jnp.float32),
                    jnp.zeros((tokens, HEAD_SIZE), jnp.float32),
                ),
            )
            o_ref[:, cols] = total / mass
            lse = top + jnp.log2(mass)
            lse_ref[...] = jnp.where(lane == h, lse, 0.0 if h == 0 else lse_ref[...])
            yield True

    return Task(
        [begin, q, kv],
        [VMEM] * 3,
        [jax.ShapeDtypeStruct(q.shape, jnp.float32), jax.ShapeDtypeStruct((tokens, HEAD_SIZE), jnp.float32)],
        [VMEM] * 2,
        [],
        None,
        run,
    )


def forward(most, count, begin, weights, rows_in, bias, cosine, sine, x, gain):
    tokens, width = rows_in.shape
    part, pre_cols = x.shape[0], bias.shape[1]
    inner = pre_cols - 2 * HEAD_SIZE
    matrix = gather(weights, count, flat=True)
    keys = gather(jax.ShapeDtypeStruct((tokens, 2 * HEAD_SIZE), jnp.bfloat16), count, flat=True)
    q = jax.ShapeDtypeStruct((tokens, inner), jnp.bfloat16)
    kv = keys.outs[0]
    core = attend(most, begin, q, kv)
    rows = gather(jax.ShapeDtypeStruct((part, width), jnp.bfloat16), count, tower=True)
    pair = swap([jax.ShapeDtypeStruct((part, width), jnp.bfloat16)])
    n_pair, n_matrix, n_keys = len(pair.scratch), len(matrix.scratch), len(keys.scratch)
    columns = 256
    skip = weights.shape[1] - inner

    def run(
        begin_ref, w_ref, in_ref, bias_ref, cos_ref, sin_ref, x_ref, gain_ref,
        attn_ref, q_ref, kv_ref, o_ref, lse_ref, hidden_ref, rows_ref, *scratch
    ):
        sent, got, normed, whole, own = scratch[:5]
        scratch = scratch[5:]
        half = lax.axis_index("head")
        yield from matrix.run(w_ref, attn_ref, *scratch[:n_matrix])
        scratch = scratch[n_matrix:]

        def turned(value):
            return value * cos_ref[...] + pltpu.roll(value, HEAD_SIZE // 2, 1) * sin_ref[...]

        def pre_of(start):
            cols = pl.ds(start, 2 * HEAD_SIZE)
            return (
                jnp.dot(in_ref[...], attn_ref[:, cols], preferred_element_type=jnp.float32) + bias_ref[:, cols]
            )

        def two_heads(i, carry):
            start = pl.multiple_of(i * 2 * HEAD_SIZE, 2 * HEAD_SIZE)
            pre = pre_of(start)
            q_ref[:, pl.ds(start, HEAD_SIZE)] = turned(pre[:, :HEAD_SIZE]).astype(q_ref.dtype)
            q_ref[:, pl.ds(start + HEAD_SIZE, HEAD_SIZE)] = turned(pre[:, HEAD_SIZE:]).astype(q_ref.dtype)
            return carry

        pre = pre_of(inner)
        own[0, :, :HEAD_SIZE] = turned(pre[:, :HEAD_SIZE]).astype(own.dtype)
        own[0, :, HEAD_SIZE:] = pre[:, HEAD_SIZE:].astype(own.dtype)
        for step, _ in enumerate(keys.run(own, kv_ref, *scratch[:n_keys])):
            if step == 0:
                lax.fori_loop(0, inner // (2 * HEAD_SIZE), two_heads, 0)
            yield True
        scratch = scratch[n_keys:]
        yield from core.run(begin_ref, q_ref, kv_ref, o_ref, lse_ref)

        def project(i, carry):
            cols = pl.ds(pl.multiple_of(i * columns, columns), columns)
            whole[:, cols] = lax.dot_general(
                o_ref[...].astype(jnp.bfloat16),
                attn_ref[cols, skip:],
                (((1,), (1,)), ((), ())),
                preferred_element_type=jnp.float32,
            )
            return carry

        lax.fori_loop(0, width // columns, project, 0)

        def of(h):
            return pl.ds(pl.multiple_of(h * part, part), part)

        sent[...] = whole[of(1 - half)].astype(jnp.bfloat16)
        yield from pair.run(sent, got, *scratch[:n_pair])
        step = 16

        def norm(i, carry):
            here = pl.ds(pl.multiple_of(i * step, step), step)
            there = pl.ds(pl.multiple_of(half * part + i * step, step), step)
            hidden = x_ref[here].astype(jnp.float32) + (whole[there] + got[here].astype(jnp.float32))
            hidden_ref[here] = hidden
            normed[0, here] = (hidden * rms_scale(hidden) * gain_ref[...]).astype(jnp.bfloat16)
            return carry

        lax.fori_loop(0, part // step, norm, 0)
        yield from rows.run(normed, rows_ref, *scratch[n_pair:])

    def targets():
        return matrix.targets() + pair.targets() + rows.targets()

    return Task(
        [begin] + matrix.inputs + [rows_in, bias, cosine, sine, x, gain],
        [VMEM] * 8,
        matrix.outs + [q, kv] + core.outs + [jax.ShapeDtypeStruct((part, width), jnp.float32)] + rows.outs,
        [VMEM] * 6 + rows.out_specs,
        [
            pltpu.VMEM((part, width), jnp.bfloat16),
            pltpu.VMEM((part, width), jnp.bfloat16),
            pltpu.VMEM((1, part, width), jnp.bfloat16),
            pltpu.VMEM((tokens, width), jnp.float32),
            pltpu.VMEM((1, tokens, 2 * HEAD_SIZE), jnp.bfloat16),
        ]
        + matrix.scratch
        + keys.scratch
        + pair.scratch
        + rows.scratch,
        targets,
        run,
    )


def attend_back(most, begin, q, kv, lse, raw, do):
    tokens, heads = q.shape[0], q.shape[1] // HEAD_SIZE
    across = (((1,), (1,)), ((), ()))
    down = (((0,), (0,)), ((), ()))

    def run(begin_ref, q_ref, kv_ref, lse_ref, raw_ref, do_ref, dq_ref, dkv_ref, delta_ref):
        low, high, first = window(most)(tokens)
        begin = begin_ref[...]
        index = first + lax.broadcasted_iota(jnp.int32, (tokens, 1), 0)
        lane = lax.broadcasted_iota(jnp.int32, (tokens, HEAD_SIZE), 1)
        key_lane = lax.broadcasted_iota(jnp.int32, (tokens, KEYS), 1)
        table = jnp.zeros((tokens, HEAD_SIZE), jnp.float32)
        for h in range(heads):
            cols = slice(h * HEAD_SIZE, (h + 1) * HEAD_SIZE)
            delta = jnp.sum(do_ref[:, cols].astype(jnp.float32) * raw_ref[:, cols], axis=1, keepdims=True)
            table = jnp.where(lane == h, delta, table)
        delta_ref[...] = table
        dq_ref[...] = jnp.zeros_like(dq_ref)
        blocks = kv_ref.shape[0] // KEYS

        def clear(block, carry):
            dkv_ref[block] = jnp.zeros((KEYS, 2 * HEAD_SIZE), dkv_ref.dtype)
            return carry

        lax.fori_loop(0, low, clear, 0)
        lax.fori_loop(high, blocks, clear, 0)

        def step(block, carry):
            start = pl.multiple_of(block * KEYS, KEYS)
            rows = pl.ds(start, KEYS)
            keys = kv_ref[rows, :HEAD_SIZE]
            values = kv_ref[rows, HEAD_SIZE:]
            at = key_lane + start
            seen = (at >= begin) & (at <= index)
            dk = jnp.zeros((KEYS, HEAD_SIZE), jnp.float32)
            dv = jnp.zeros((KEYS, HEAD_SIZE), jnp.float32)
            for h in range(heads):
                cols = slice(h * HEAD_SIZE, (h + 1) * HEAD_SIZE)
                q = q_ref[:, cols]
                do = do_ref[:, cols]
                scores = lax.dot_general(q, keys, across, preferred_element_type=jnp.float32)
                probs = jnp.where(seen, jnp.exp2(scores * SCALE2 - lse_ref[:, h : h + 1]), 0.0)
                pull = lax.dot_general(do, values, across, preferred_element_type=jnp.float32)
                ds = (probs * (pull - delta_ref[:, h : h + 1])).astype(jnp.bfloat16)
                dq_ref[:, cols] += jnp.dot(ds, keys, preferred_element_type=jnp.float32)
                dk = dk + lax.dot_general(ds, q, down, preferred_element_type=jnp.float32)
                dv = dv + lax.dot_general(
                    probs.astype(jnp.bfloat16), do, down, preferred_element_type=jnp.float32
                )
            dkv_ref[block, :, :HEAD_SIZE] = (dk * SCALE).astype(dkv_ref.dtype)
            dkv_ref[block, :, HEAD_SIZE:] = dv.astype(dkv_ref.dtype)
            return carry

        parts = 3
        reach = high - low
        yield True
        for i in range(parts):
            lax.fori_loop(low + reach * i // parts, low + reach * (i + 1) // parts, step, 0)
            yield True

    return Task(
        [begin, q, kv, lse, raw, do],
        [VMEM] * 6,
        [
            jax.ShapeDtypeStruct(q.shape, jnp.float32),
            jax.ShapeDtypeStruct((kv.shape[0] // KEYS, KEYS, kv.shape[1]), kv.dtype),
        ],
        [VMEM] * 2,
        [pltpu.VMEM((tokens, HEAD_SIZE), jnp.float32)],
        None,
        run,
    )


def doc_layout(row_lengths, first_token, token_count):
    doc_ends = jnp.cumsum(row_lengths)
    doc_starts = doc_ends - row_lengths
    token_index = first_token + jnp.arange(token_count, dtype=jnp.int32)
    doc_begin = jnp.max(
        jnp.where(doc_starts[None, :] <= token_index[:, None], doc_starts[None, :], 0), axis=1
    )
    return (doc_begin, token_index - doc_begin)


def rope_tables(positions):
    freq = rope_base ** (-jnp.arange(0, HEAD_SIZE, 2, dtype=jnp.float32) / HEAD_SIZE)
    angle = positions.astype(jnp.float32)[:, None] * freq[None, :]
    angle = jnp.concatenate([angle, angle], axis=1)
    return (jnp.cos(angle)[:, None, :], jnp.sin(angle)[:, None, :])


def rotary_apply(values, cosine_table, sine_table):
    half_width = values.shape[-1] // 2
    turned = jnp.concatenate([-values[..., half_width:], values[..., :half_width]], axis=-1)
    return values * cosine_table + turned * sine_table


def unrotate(grads, cosine_table, sine_table):
    half_width = grads.shape[-1] // 2
    scaled_grad = grads * sine_table
    back_part = jnp.concatenate(
        [scaled_grad[..., half_width:], -scaled_grad[..., :half_width]], axis=-1
    )
    return grads * cosine_table + back_part


def rms_scale(values):
    return lax.rsqrt(jnp.mean(values * values, axis=-1, keepdims=True) + norm_epsilon)


def norm_back(grad_out, inputs, scale, gain):
    weighted = grad_out * gain
    return scale * weighted - inputs * scale**3 * jnp.mean(
        weighted * inputs, axis=-1, keepdims=True
    )


def dot(a, b, dims=((1,), (0,))):
    return lax.dot_general(a, b, (dims, ((), ())), preferred_element_type=jnp.float32)


across_dims = ((1,), (1,))
token_dims = ((0,), (0,))


def backward(most, count, begin, q, kv, lse, raw, own, attn):
    tokens, width = q.shape[0], own.shape[1]
    part, inner = own.shape[0], q.shape[1]
    core = attend_back(most, begin, q, kv, lse, raw, jax.ShapeDtypeStruct(q.shape, jnp.bfloat16))
    d_query, d_kv = core.outs
    sums = scatter(jax.ShapeDtypeStruct((kv.shape[0], kv.shape[1]), kv.dtype), count)
    columns = 256
    skip = attn.shape[1] - inner

    def run(
        begin_ref, q_ref, kv_ref, lse_ref, raw_ref, own_ref, attn_ref, dq_ref, sums_ref, branch_ref, delta, do, dkv, send, recv, *scratch
    ):
        half = lax.axis_index("head")
        here = pl.ds(pl.multiple_of(half * part, part), part)
        copy = remote(
            own_ref, branch_ref.at[here], send, recv, {"dp": lax.axis_index("dp"), "head": 1 - half}
        )
        copy.start()
        branch_ref[here] = own_ref[...]
        yield True
        copy.wait_recv()

        def project(i, carry):
            cols = pl.ds(pl.multiple_of(i * columns, columns), columns)
            there = pl.ds(pl.multiple_of(skip + i * columns, columns), columns)
            do[:, cols] = jnp.dot(
                branch_ref[...], attn_ref[:, there], preferred_element_type=jnp.float32
            ).astype(do.dtype)
            return carry

        lax.fori_loop(0, inner // columns, project, 0)
        yield from core.run(begin_ref, q_ref, kv_ref, lse_ref, raw_ref, do, dq_ref, dkv, delta)
        yield from sums.run(dkv, sums_ref, *scratch)
        copy.wait_send()

    def targets():
        return [("half", True, {"dp": lax.axis_index("dp"), "head": 1 - lax.axis_index("head")})] + sums.targets()

    return Task(
        [begin, q, kv, lse, raw, own, attn],
        [VMEM] * 7,
        [d_query] + sums.outs + [jax.ShapeDtypeStruct((tokens, width), jnp.bfloat16)],
        [VMEM] * 3,
        core.scratch
        + [pltpu.VMEM(q.shape, jnp.bfloat16), pltpu.VMEM(d_kv.shape, d_kv.dtype), dma, dma]
        + sums.scratch,
        targets,
        run,
    )


def weight_grads(rows, grads, d_gate, d_up, active, weights):
    arrays = [rows, grads, d_gate, d_up, active, weights]
    width, units, tokens = rows.shape[1], active.shape[1], rows.shape[0]
    columns = 256
    down = (((0,), (0,)), ((), ()))
    across = (((1,), (1,)), ((), ()))

    def run(*refs):
        ins, (o_ref, out_ref), held, (sems,) = refs[:6], refs[6:8], refs[8:14], refs[14:]
        sources = list(ins[:5]) + [ins[5].at[2]]
        copies = [pltpu.make_async_copy(sources[i], held[i], sems.at[i]) for i in range(6)]
        for i in (4, 5, 0, 2, 3, 1):
            copies[i].start()
        yield True
        for i in (4, 5):
            copies[i].wait()

        def forth(i, carry):
            here = pl.ds(pl.multiple_of(i * columns, columns), columns)
            out_ref[here] = lax.dot_general(
                held[4][here], held[5][...], across, preferred_element_type=jnp.float32
            ).astype(out_ref.dtype)
            return carry

        lax.fori_loop(0, tokens // columns, forth, 0)
        yield True
        for i in (0, 2, 3):
            copies[i].wait()

        def first(i, carry):
            cols = pl.ds(pl.multiple_of(i * columns, columns), columns)
            for kind in (0, 1):
                o_ref[kind, cols] = lax.dot_general(
                    held[0][:, cols], held[2 + kind][...], down, preferred_element_type=jnp.float32
                ).astype(o_ref.dtype)
            return carry

        def second(i, carry):
            cols = pl.ds(pl.multiple_of(i * columns, columns), columns)
            o_ref[2, cols] = lax.dot_general(
                held[1][:, cols], held[4][...], down, preferred_element_type=jnp.float32
            ).astype(o_ref.dtype)
            return carry

        half = width // columns // 2
        lax.fori_loop(0, half, first, 0)
        yield True
        lax.fori_loop(half, width // columns, first, 0)
        yield True
        copies[1].wait()
        lax.fori_loop(0, width // columns, second, 0)
        yield True

    return Task(
        arrays,
        [HBM] * 6,
        [jax.ShapeDtypeStruct((3, width, units), jnp.bfloat16), jax.ShapeDtypeStruct((tokens, width), jnp.bfloat16)],
        [VMEM] * 2,
        [pltpu.VMEM(a.shape, a.dtype) for a in arrays[:5]] + [pltpu.VMEM((width, units), weights.dtype), dma((6,))],
        None,
        run,
    )


def longest(token_count):
    return 2048 if token_count == 4096 else token_count


def body(
    count,
    layer_in,
    gain_attn,
    q_weight,
    q_bias,
    key_weight,
    key_bias,
    value_weight,
    value_bias,
    o_weight,
    gain_mlp,
    gate_weight,
    up_weight,
    down_weight,
    row_lengths,
    source_ids,
    source_weights,
    out_grad,
):
    f32, bf16 = jnp.float32, jnp.bfloat16
    tok_rows, width = layer_in.shape
    part = tok_rows // 2
    half = lax.axis_index("head")
    first_token = lax.axis_index("dp") * tok_rows
    doc_begin, positions = doc_layout(row_lengths, first_token, tok_rows)
    cosine_table, sine_table = rope_tables(positions)
    q_cols = q_weight.shape[1]
    kv_cols = key_weight.shape[1]
    heads = q_cols // HEAD_SIZE
    ff_cols = gate_weight.shape[1]

    def mine(rows):
        return lax.dynamic_slice_in_dim(rows, half * part, part, 0)

    def other(rows):
        return lax.dynamic_slice_in_dim(rows, (1 - half) * part, part, 0)

    def join(own, peer):
        return jnp.where(half == 0, jnp.concatenate([own, peer]), jnp.concatenate([peer, own]))

    attn_local = jnp.concatenate([q_weight, key_weight, value_weight, o_weight.T], axis=1)
    picked = source_ids[:, None] == jnp.arange(source_weights.shape[0], dtype=jnp.int32)[None, :]
    row_scale = (
        jnp.sum(jnp.where(picked, source_weights[None, :], 0), axis=1).astype(f32) / loss_denominator
    )
    cotangent = mine(out_grad).astype(f32) * mine(row_scale[:, None])
    qkv_cols = q_cols + 2 * kv_cols
    inputs = layer_in.astype(f32)
    scale_one = rms_scale(inputs)
    gain_one = gain_attn.astype(f32)
    normed = (inputs * scale_one * gain_one).astype(bf16)
    bias = jnp.concatenate([q_bias, key_bias, value_bias]).astype(f32)
    begin = doc_begin[:, None].astype(jnp.int32)
    most = longest(count * tok_rows)
    mlp_local = jnp.stack([gate_weight, up_weight, down_weight.T])
    gain_two = gain_mlp.astype(f32)
    signed_sine = jnp.concatenate([-sine_table[:, 0, : HEAD_SIZE // 2], sine_table[:, 0, HEAD_SIZE // 2 :]], axis=1)
    ahead = (
        (1,) * 8 + (0,) + (1,) * 7 + (0,) + (1,) * 7 + (0, 2, 0)
        + (1,) * 8 + (0,) + (1,) * 14 + (2, 2, 2, 1)
        + (1, 0, 1, 2, 2, 0, 1, 0, 2, 2, 1, 2, 2, 2, 0, 1, 2, 2, 2, 1, 2, 2, 0)
        + (1, 2, 2, 2, 1) + (1, 2) * 24
    )
    ((mlp_full,), (attn_full, query_rows, kv_all, attended_raw, row_lse, hidden, rows_all), (grad_all,)) = fuse(
        3,
        "forward",
        spread(mlp_local, count),
        forward(
            most,
            count,
            begin,
            attn_local,
            normed,
            bias[None, :],
            cosine_table[:, 0, :],
            signed_sine,
            mine(layer_in),
            gain_two[None, :],
        ),
        gather(cotangent.astype(bf16), count, tower=True),
        order=ahead,
    )
    grad_all = grad_all.reshape(-1, width)
    full_qkv = attn_full[:, :qkv_cols]
    attended = attended_raw.astype(bf16)
    scale_two = rms_scale(hidden)
    rows_all = rows_all.reshape(-1, width)

    full_gate, full_up, full_down = mlp_full[0], mlp_full[1], mlp_full[2]
    gate_act = dot(rows_all, full_gate)
    up_act = dot(rows_all, full_up)
    sigmoid_gate = jax.nn.sigmoid(gate_act)
    silu_gate = gate_act * sigmoid_gate
    active = (silu_gate * up_act).astype(bf16)
    d_active = dot(grad_all, full_down)
    d_gate = (d_active * up_act * sigmoid_gate * (1.0 + gate_act * (1.0 - sigmoid_gate))).astype(bf16)
    d_up = (d_active * silu_gate).astype(bf16)
    norm_two_part = (dot(d_gate, full_gate, across_dims) + dot(d_up, full_up, across_dims)).astype(bf16)

    if count <= 16:
        ((d_normed_mlp,), (mlp_grads, mlp_part)) = fuse(
            8,
            "scatter_grads",
            scatter(norm_two_part, count, tower=True),
            weight_grads(rows_all, grad_all, d_gate, d_up, active, mlp_full),
            order=(0, 1, 0, 0, 1, 0, 0, 1, 0, 1, 0, 1),
        )
    else:
        d_normed_mlp = scatter_all(norm_two_part, count, 8, "scatter_rows", tower=True)
        mlp_part = dot(active, full_down, across_dims).astype(bf16)
        mlp_grads = jnp.stack(
            [
                dot(rows_all, d_gate, token_dims).astype(bf16),
                dot(rows_all, d_up, token_dims).astype(bf16),
                dot(grad_all, active, token_dims).astype(bf16),
            ]
        )
    gain_two_local = jnp.sum(d_normed_mlp * hidden * scale_two, axis=0)
    d_hidden = cotangent + norm_back(d_normed_mlp, hidden, scale_two, gain_two)
    branch_own = d_hidden.astype(bf16)
    tasks = [
        collect(mlp_grads, count, ff_cols),
        backward(most, count, begin, query_rows, kv_all, row_lse, attended_raw, branch_own, attn_full),
    ]
    turns = (1, 0, 1, 1, 0, 1, 0, 1, 0, 1, 1, 0)
    if count <= 16:
        tasks.append(scatter(mlp_part, count, tower=True))
        turns = (1, 0) + (2,) * 5 + (1, 0, 1, 2, 0, 1, 2, 0, 1, 2, 0, 1) + (1,) * 4 + (0, 2)
    found = fuse(17, "backward_collect", *tasks, order=turns)
    ((mlp_part_sums,), (d_query, kv_sums, branch_grad)) = found[:2]
    mlp_out = found[2][0] if count <= 16 else scatter_all(mlp_part, count, 25, "scatter_out", tower=True)
    layer_out_own = (hidden + mlp_out).astype(bf16)
    mlp_part_sums = mlp_part_sums.astype(f32)
    out_proj_grad = dot(branch_grad, attended, token_dims)
    d_queries = (d_query * SCALE).astype(bf16).astype(f32)
    d_key_rot = kv_sums[:, :kv_cols].astype(bf16).astype(f32)
    d_value_rows = kv_sums[:, kv_cols:].astype(bf16)
    d_turned = jnp.concatenate([d_queries, d_key_rot], axis=1).reshape(tok_rows, heads + 1, HEAD_SIZE)
    d_pre = jnp.concatenate(
        [
            unrotate(d_turned, cosine_table, sine_table).reshape(tok_rows, q_cols + kv_cols).astype(bf16),
            d_value_rows,
        ],
        axis=1,
    )
    bias_local = jnp.sum(d_pre.astype(f32), axis=0)
    qkv_grad = dot(normed, d_pre, token_dims)
    attn_grads = jnp.concatenate([qkv_grad, out_proj_grad], axis=1).astype(bf16)
    norm_one_part = dot(d_pre, full_qkv, across_dims)
    norm_send = other(norm_one_part).astype(bf16)
    exchange = swap([norm_send, layer_out_own])
    if count <= 16:
        ((attn_part,), (norm_peer, layer_out_peer)) = fuse(21, "scatter_last", scatter(attn_grads, count), exchange)
    else:
        attn_part = scatter_all(attn_grads, count, 21, "scatter_attn")
        ((norm_peer, layer_out_peer),) = fuse(33, "swap_norm", exchange)
    d_normed = mine(norm_one_part) + norm_peer.astype(f32)
    inputs_own = mine(inputs)
    scale_own = mine(scale_one)
    gain_one_local = jnp.sum(d_normed * inputs_own * scale_own, axis=0)
    layer_in_grad_own = (d_hidden + norm_back(d_normed, inputs_own, scale_own, gain_one)).astype(bf16)

    small = jnp.concatenate([bias_local, gain_one_local, gain_two_local]).reshape(-1, LANES)
    ((small_all,), (layer_in_grad_peer,)) = fuse(
        34, "gather_sums", gather(small, count, both=True), swap([layer_in_grad_own])
    )
    small_all = small_all.reshape(count, 2, -1)
    small_sum = jnp.sum(small_all[:, 0], axis=0)
    gains = (small_sum[qkv_cols:] + jnp.sum(small_all[:, 1, qkv_cols:], axis=0)).reshape(2, width)
    layer_in_grad = join(layer_in_grad_own, layer_in_grad_peer)
    layer_out = join(layer_out_own, layer_out_peer)
    return (
        layer_out,
        layer_in_grad,
        gains[0],
        attn_part[:, :q_cols],
        small_sum[:q_cols],
        attn_part[:, q_cols : q_cols + kv_cols],
        small_sum[q_cols : q_cols + kv_cols],
        attn_part[:, q_cols + kv_cols : qkv_cols],
        small_sum[q_cols + kv_cols : qkv_cols],
        attn_part[:, qkv_cols:].T,
        gains[1],
        mlp_part_sums[0],
        mlp_part_sums[1],
        mlp_part_sums[2].T,
    )


def solution(mesh):
    placed = (
        P("dp", None),
        P(),
        P("dp", "head"),
        P("head"),
        P("dp", "head"),
        P("head"),
        P("dp", "head"),
        P("head"),
        P("head", "dp"),
        P(),
        P("dp", "head"),
        P("dp", "head"),
        P("head", "dp"),
        P(),
        P("dp"),
        P(),
        P("dp", None),
    )
    return jax.shard_map(
        functools.partial(body, mesh.shape["dp"]),
        mesh=mesh,
        in_specs=placed,
        out_specs=(
            P("dp", None),
            P("dp", None),
            P(),
            P("dp", "head"),
            P("head"),
            P("dp", "head"),
            P("head"),
            P("dp", "head"),
            P("head"),
            P("head", "dp"),
            P(),
            P("dp", "head"),
            P("dp", "head"),
            P("head", "dp"),
        ),
        check_vma=False,
    )
```
